256 devices in a mesh: dp: 128 (over z, x, y), grp: 2 (over core).
Axes of the slice: x: 4, y: 4, z: 8, core: 2. Of those that a mesh axis runs over, the one named last changes fastest.
Arguments:
- embeds: bfloat16 [65536, 1024], P(('dp', 'grp')), may hold values from -7 to 7
- quality: float32 [65536], P(('dp', 'grp')), may hold values from 0.5 to 2
- domain_ids: int32 [65536], P(('dp', 'grp')), may hold values from 0 to 15, as said below
- domain_weight: float32 [16], replicated, may hold values from 0.5 to 2
- dest: int32 [65536], P(('dp', 'grp')), may hold values from 0 to 255, as said below
- counts: int32 [256], P(('dp', 'grp')), may hold values from 192 to 256, as said below
- winners: int32 [4], replicated, may hold values from 0 to 65535, as said below
Outputs:
- relaid: bfloat16 [131072, 1024], P(('dp', 'grp'))
- residual_gain: float32 [131072], P(('dp', 'grp'))
- chol_rows: float32 [4, 131072], P(None, ('dp', 'grp'))
The draws below stay inside these ranges and needn't reach their ends.
Inputs may be any that keep to these rules, and one draw needn't show every extreme that they name: Rows 0 to counts - 1 of a device are valid, and one device has 256 valid rows. `dest`: destination device over dp and grp (index over dp+grp); among the valid rows of one device at most 2 name any one destination, and on every device some destination is named by exactly 2 valid rows. `domain_ids`: non-decreasing within each device's rows; a device's rows carry one domain number or two consecutive ones. `winners`: distinct valid rows, on distinct devices.
All inputs are finite; a program needn't handle non-finite values.
Results may differ from the reference program's by a relative error of at most 0.0048.
The reference program's roundings to bfloat16 on the way (of `row_quality` and `bal_quality`) count: a program that leaves them out, or rounds other values in their place, can miss the bound.
Values may be sent and summed in bfloat16 or wider, within the bound.
No kernel may reach another device: no remote copies, remote signals or barrier semaphores. Data moves between devices by JAX's collectives and lax.ppermute only.
A program may use at most 64 MiB of HBM per device.

```python
import math
import jax
import jax.numpy as jnp
from jax import lax

D = 1024
DOMAINS = 16
STEPS = 4
SLOTS = 256
SHARDS = 256
CAP = 2
ROWS_BAL = 512
TOTAL_IN = 65536
TOTAL_OUT = 131072
N_DP = 128
N_GRP = 2


def device_counts(key):
    inner_key = jax.random.fold_in(key, 11)
    key_first, key_second = jax.random.split(inner_key)
    base_counts = jax.random.randint(key_first, (SHARDS,), SLOTS // 4 * 3, SLOTS + 1)
    busiest = jax.random.randint(key_second, (), 0, SHARDS)
    device_index = jnp.arange(SHARDS)
    full_rows = (device_index == busiest) | (device_index == SHARDS - 1)
    return jnp.where(full_rows, SLOTS, base_counts).astype(jnp.int32)


def domain_layout(key):
    inner_key = jax.random.fold_in(key, 13)
    lower_domain = jnp.arange(SHARDS) * DOMAINS // SHARDS
    upper_domain = jnp.minimum(lower_domain + 1, DOMAINS - 1)
    split_row = jax.random.randint(inner_key, (SHARDS, 1), 0, SLOTS + 1)
    column_index = jnp.arange(SLOTS)[None, :]
    layout = jnp.where(column_index >= split_row, upper_domain[:, None], lower_domain[:, None])
    return layout.reshape(-1).astype(jnp.int32)


def draw_counts(key, part):
    return device_counts(key)


def draw_domain_ids(key, part):
    return domain_layout(key)


def draw_embeds(key, part):
    inner_key = jax.random.fold_in(key, 17)
    key_list = jax.random.split(inner_key, 3)
    shared = jnp.clip(jax.random.normal(key_list[0], (D,), jnp.float32), -4.0, 4.0)
    centres = jnp.clip(jax.random.normal(key_list[1], (DOMAINS, D), jnp.float32), -4.0, 4.0)
    noise = jnp.clip(jax.random.normal(key_list[2], (SHARDS * SLOTS, D), jnp.float32), -4.0, 4.0)
    domains = domain_layout(key)
    values = 0.5 * shared[None, :] + 0.7 * centres[domains] + 0.5 * noise
    return values.astype(jnp.bfloat16)


def draw_dest(key, part):
    inner_key = jax.random.fold_in(key, 19)
    key_list = jax.random.split(inner_key, SHARDS)

    def one_device(device_key):
        key_first, key_second, key_third = jax.random.split(device_key, 3)
        target = jax.random.randint(key_first, (), 0, SHARDS)
        labels = (jnp.arange(SHARDS * CAP) // CAP + target) % SHARDS
        shuffled = jax.random.permutation(key_second, labels[CAP:])
        row_labels = jnp.concatenate([labels[:CAP], shuffled])[:SLOTS]
        head_part = jax.random.permutation(key_third, row_labels[:SLOTS // 4])
        return jnp.concatenate([head_part, row_labels[SLOTS // 4:]])
    return jax.vmap(one_device)(key_list).reshape(-1).astype(jnp.int32)


def draw_winners(key, part):
    valid_counts = device_counts(key)
    inner_key = jax.random.fold_in(key, 23)
    key_first, key_second, key_third = jax.random.split(inner_key, 3)
    middle = 1 + jax.random.permutation(key_first, SHARDS - 2)[:STEPS - 2]
    owners = jnp.concatenate([jnp.array([0, SHARDS - 1], jnp.int32), middle.astype(jnp.int32)])
    random_rows = jax.random.randint(key_second, (STEPS,), 0, valid_counts[owners])
    position = jnp.arange(STEPS)
    picked_rows = jnp.where(position == 0, 0, jnp.where(position == 1, SLOTS - 1, random_rows))
    order = jax.random.permutation(key_third, STEPS)
    return (owners * SLOTS + picked_rows)[order].astype(jnp.int32)


def shard_levels(own_key, extent, pieces, least, top_value):
    level = 1.0
    for axis_at, shards_of in pieces:
        draws = jax.random.uniform(jax.random.fold_in(jax.random.fold_in(own_key, 6), axis_at), (shards_of,), jnp.float32, least / len(pieces), top_value / len(pieces))
        level = level * jnp.repeat(jnp.exp(draws), extent[axis_at] // shards_of).reshape((-1,) + (1,) * (len(extent) - 1 - axis_at))
    return level


def setup_inputs(seed: int = 0) -> dict:
    arg_keys = jax.random.split(jax.random.key(seed), 8)
    embeds = draw_embeds(jax.random.fold_in(arg_keys[7], 71), 0)
    quality = jnp.clip(jnp.exp(math.log(2.0) - 1.3862944 * jax.random.uniform(arg_keys[1], (TOTAL_IN,), jnp.float32) ** shard_levels(arg_keys[1], (TOTAL_IN,), ((0, 256),), -0.2, 0.2)), 0.5, 2.0)
    domain_ids = draw_domain_ids(jax.random.fold_in(arg_keys[7], 71), 0)
    domain_weight = jnp.clip(jnp.exp(jax.random.uniform(arg_keys[3], (DOMAINS,), jnp.float32, math.log(0.5), math.log(2.0))), 0.5, 2.0)
    dest = draw_dest(jax.random.fold_in(arg_keys[7], 71), 0)
    counts = draw_counts(jax.random.fold_in(arg_keys[7], 71), 0)
    winners = draw_winners(jax.random.fold_in(arg_keys[7], 71), 0)
    return {"embeds": embeds, "quality": quality, "domain_ids": domain_ids, "domain_weight": domain_weight, "dest": dest, "counts": counts, "winners": winners}


RIDGE = 0.1

def reference(embeds, quality, domain_ids, domain_weight, dest, counts, winners):
    shards = N_DP * N_GRP
    row_quality = (quality * domain_weight[domain_ids]).astype(jnp.bfloat16)
    dest_grid = dest.reshape(shards, SLOTS)
    row_index = jnp.arange(SLOTS, dtype=jnp.int32)
    is_valid = row_index[None, :] < counts[:, None]
    targets = jnp.arange(shards, dtype=jnp.int32)

    def rank_rows(pair):
        dest_row, valid_row = pair
        dest_hot = ((dest_row[:, None] == targets[None, :]) & valid_row[:, None]).astype(jnp.int32)
        running = jnp.cumsum(dest_hot, axis=0) - dest_hot
        return lax.optimization_barrier(jnp.sum(running * dest_hot, axis=1)).astype(jnp.int32)
    dest_rank = lax.map(rank_rows, (dest_grid, is_valid))
    source_ids = jnp.arange(shards, dtype=jnp.int32)[:, None]
    bal_place = dest_grid * ROWS_BAL + source_ids * CAP + dest_rank
    bal_place = jnp.where(is_valid, bal_place, TOTAL_OUT).reshape(-1).astype(jnp.int32)
    relaid = jnp.zeros((TOTAL_OUT, D), jnp.bfloat16).at[bal_place].set(embeds, mode='drop')
    bal_quality = jnp.zeros((TOTAL_OUT,), jnp.bfloat16).at[bal_place].set(row_quality, mode='drop').astype(jnp.float32)
    win_rows = embeds[winners]
    win_place = bal_place[winners]
    blocks = relaid.reshape(shards, ROWS_BAL, D)

    def measure(block):
        row_norms = lax.optimization_barrier(jnp.sum(jnp.square(block.astype(jnp.float32)), axis=1))
        kernel_dots = lax.dot_general(win_rows, block, (((1,), (1,)), ((), ())), preferred_element_type=jnp.float32)
        return (row_norms, kernel_dots)
    row_norms, kernel_dots = lax.map(measure, blocks)
    row_norms = row_norms.reshape(-1)
    kernel_dots = jnp.transpose(kernel_dots, (1, 0, 2)).reshape(STEPS, TOTAL_OUT)
    residual_gain = jnp.where(bal_quality > 0, bal_quality * bal_quality * row_norms / D + RIDGE, 0.0)
    all_index = jnp.arange(TOTAL_OUT, dtype=jnp.int32)
    chol_rows = jnp.zeros((STEPS, TOTAL_OUT), jnp.float32)
    for turn_index in range(STEPS):
        target = win_place[turn_index]
        win_quality = bal_quality[target]
        ridge_hit = jnp.where(all_index == target, RIDGE, 0.0)
        column = bal_quality * win_quality * kernel_dots[turn_index] / D + ridge_hit
        win_chol = chol_rows[:, target]
        inner_sum = lax.optimization_barrier(jnp.sum(chol_rows * win_chol[:, None], axis=0))
        root_gain = jnp.sqrt(residual_gain[target])
        new_entry = (column - inner_sum) / root_gain
        chol_rows = chol_rows.at[turn_index].set(new_entry)
        residual_gain = residual_gain - new_entry * new_entry
    return (relaid, residual_gain, chol_rows)
```

```python
import jax
import jax.numpy as jnp
from jax import lax
from jax.experimental import pallas as pl
from jax.experimental.pallas import tpu as pltpu
from jax.sharding import Mesh
from jax.sharding import PartitionSpec as P

ALL = ("z", "x", "y", "core")
PLANE = ("x", "y", "core")
RING = ("x", "y", "core", "z")
RIDGE = 0.1
LANES = 128
F32 = jnp.float32
BF16 = jnp.bfloat16
VMEM = pl.BlockSpec(memory_space=pltpu.VMEM)
SMEM = pl.BlockSpec(memory_space=pltpu.SMEM)


def iota(shape, dim):
    return lax.broadcasted_iota(jnp.int32, shape, dim)


def prep(shards, plane, rel, counts, weight, emb, dest, quality, domain, slot_out, aux_out, picks):
    slots, width = emb.shape
    steps = rel.shape[0]
    square = (slots, slots)
    row, col = iota(square, 0), iota(square, 1)
    dest_row = dest[...].astype(F32)
    across = jnp.broadcast_to(dest_row, square)
    down = jnp.sum(jnp.where(row == col, across, 0.0), axis=1, keepdims=True)
    earlier = (down == across) & (row < col)
    rank = jnp.sum(jnp.where(earlier, 1.0, 0.0), axis=0, keepdims=True)
    lane = iota((1, slots), 1)
    valid = lane < counts[0]
    ring = shards // plane
    to = dest[...]
    to = lax.rem(to, plane) * ring + lax.div(to, plane)
    slot = jnp.where(valid, 2.0 * to.astype(F32) + rank, -1.0)
    slot_out[...] = slot.astype(jnp.int32)
    scale = jnp.zeros((1, slots), F32)
    for k in range(weight.shape[0]):
        scale = jnp.where(domain[...] == k, weight[k], scale)
    row_quality = (quality[...] * scale).astype(BF16).astype(F32)

    peer = (iota((shards, slots), 0) * 2).astype(F32)
    first = jnp.sum(jnp.where(slot == peer, row_quality, 0.0), axis=1, keepdims=True)
    second = jnp.sum(jnp.where(slot == peer + 1.0, row_quality, 0.0), axis=1, keepdims=True)

    turn = iota((8, slots), 0)
    wanted = jnp.full((8, slots), -1, jnp.int32)
    for t in range(steps):
        wanted = jnp.where(turn == t, rel[t], wanted)
    chosen = (iota((8, slots), 1) == wanted) & valid
    spread = jnp.zeros((8, LANES), F32)
    turn_out, lane_out = iota((8, LANES), 0), iota((8, LANES), 1)
    for k, value in enumerate((row_quality, dest_row, rank)):
        mine = jnp.sum(jnp.where(chosen, value, 0.0), axis=1, keepdims=True)
        here = (lane_out == turn_out + (2 + k * steps)) & (turn_out < steps)
        spread = spread + jnp.where(here, mine, 0.0)
    scalars = jnp.sum(spread, axis=0, keepdims=True)
    lanes = iota((shards, LANES), 1)
    side = jnp.where(lanes == 0, first, jnp.where(lanes == 1, second, scalars))

    picked = jnp.dot(chosen.astype(F32).astype(BF16), emb[...], preferred_element_type=F32)
    parts = width // LANES
    for t in range(steps):
        for j in range(parts):
            picks[t * parts + j : t * parts + j + 1, :] = picked[t : t + 1, j * LANES : (j + 1) * LANES]
    spot = iota((shards, plane), 0) - ring * iota((shards, plane), 1)
    share = ((spot >= 0) & (spot < ring)).astype(F32).astype(BF16)
    piece = jnp.dot(share, picks[...].astype(BF16), preferred_element_type=F32)
    aux_out[:, :LANES] = piece.astype(BF16)
    aux_out[:, LANES:] = side.astype(BF16)


def place_rows(slot, emb, out):
    rows = out.shape[0]
    slots = slot.shape[1]
    block = 128
    for at in range(0, rows, block):
        hot = (iota((block, slots), 0) + at) == slot[...]
        hot = hot.astype(F32).astype(BF16)
        out[at : at + block, :] = jnp.dot(hot, emb[...], preferred_element_type=F32).astype(BF16)


def select(ring, winners, base, rows, pieces, side, gain_out, chol_out, wide):
    balanced, width = rows.shape
    steps = chol_out.shape[0]
    shards = side.shape[0]
    parts = width // LANES
    wide[...] = jnp.zeros_like(wide)
    piece = pieces[...].astype(F32)
    for t in range(steps):
        for j in range(parts):
            wide[t : t + 1, j * LANES : (j + 1) * LANES] = piece[t * parts + j : t * parts + j + 1, :]
    win = wide[...].astype(BF16)
    nt = (((1,), (1,)), ((), ()))
    dots = lax.dot_general(win, rows[...], nt, preferred_element_type=F32)
    gram = lax.dot_general(win, win, nt, preferred_element_type=F32)
    partial = jnp.zeros((balanced, LANES), F32)
    for j in range(parts):
        x = rows[:, j * LANES : (j + 1) * LANES].astype(F32)
        partial = partial + x * x
    ones = jnp.ones((8, LANES), BF16)
    norms = jnp.zeros((8, balanced), F32)
    rest = partial
    for _ in range(3):
        part = rest.astype(BF16)
        rest = rest - part.astype(F32)
        norms = norms + lax.dot_general(ones, part, nt, preferred_element_type=F32)
    norms = norms[0:1, :]

    received = side[...].astype(F32)
    grid = (shards, balanced)
    source, slot = iota(grid, 0), iota(grid, 1)
    source = lax.rem(source, ring) * (shards // ring) + lax.div(source, ring)
    own = jnp.where(slot == 2 * source, received[:, 0:1], 0.0) + jnp.where(slot == 2 * source + 1, received[:, 1:2], 0.0)
    quality = jnp.sum(own, axis=0, keepdims=True)
    scalars = jnp.sum(received, axis=0, keepdims=True)
    win_quality = [scalars[:, 2 + t : 3 + t] for t in range(steps)]
    win_dest = [scalars[:, 2 + steps + t : 3 + steps + t].astype(jnp.int32) for t in range(steps)]
    win_rank = [scalars[:, 2 + 2 * steps + t : 3 + 2 * steps + t].astype(jnp.int32) for t in range(steps)]

    gain = jnp.where(quality > 0, quality * quality * norms / width + RIDGE, 0.0)
    local = iota((1, balanced), 1) + base[0]
    columns, roots, chol = [], [], []
    for t in range(steps):
        column = []
        for k in range(t):
            cross = win_quality[k] * win_quality[t] * gram[k : k + 1, t : t + 1] / width
            for e in range(k):
                cross = cross - columns[k][e] * column[e]
            column.append(cross / roots[k])
        own_gain = win_quality[t] * win_quality[t] * gram[t : t + 1, t : t + 1] / width + RIDGE
        for k in range(t):
            own_gain = own_gain - column[k] * column[k]
        root = jnp.sqrt(own_gain)
        inner = jnp.zeros((1, balanced), F32)
        for k in range(t):
            inner = inner + chol[k] * column[k]
        place = win_dest[t] * balanced + winners[t] // (balanced // 2) * 2 + win_rank[t]
        hit = jnp.where(local == place, RIDGE, 0.0)
        entry = (quality * win_quality[t] * dots[t : t + 1, :] / width + hit - inner) / root
        gain = gain - entry * entry
        columns.append(column)
        roots.append(root)
        chol.append(entry)
        chol_out[t : t + 1, :] = entry
    gain_out[...] = gain


def body(embeds, quality, domain_ids, domain_weight, dest, counts, winners):
    shards = lax.axis_size(ALL)
    plane = lax.axis_size(PLANE)
    slots, width = embeds.shape
    steps = winners.shape[0]
    balanced = 2 * slots
    ring = shards // plane
    me = lax.axis_index(ALL)

    slot, aux = pl.pallas_call(
        lambda *refs: prep(shards, plane, *refs),
        in_specs=[SMEM, SMEM, SMEM, VMEM, VMEM, VMEM, VMEM],
        out_specs=[VMEM, VMEM],
        out_shape=[
            jax.ShapeDtypeStruct((1, slots), jnp.int32),
            jax.ShapeDtypeStruct((shards, 2 * LANES), BF16),
        ],
        scratch_shapes=[pltpu.VMEM((plane, LANES), F32)],
        name="prep",
    )(
        winners - me * slots,
        counts,
        domain_weight,
        embeds,
        dest.reshape(1, slots),
        quality.reshape(1, slots),
        domain_ids.reshape(1, slots),
    )
    side_in = lax.all_to_all(aux.reshape(shards, 2, LANES), RING, 0, 0, tiled=True)
    send = pl.pallas_call(
        place_rows,
        in_specs=[VMEM, VMEM],
        out_specs=VMEM,
        out_shape=jax.ShapeDtypeStruct((balanced, width), BF16),
        name="place_rows",
        cost_estimate=pl.CostEstimate(flops=2 * balanced * slots * width, bytes_accessed=1 << 21, transcendentals=0),
    )(slot, embeds)
    rows_in = lax.all_to_all(send.reshape(shards, 2, width), RING, 0, 0, tiled=True)
    piece = jnp.sum(side_in[:, 0, :].astype(F32), axis=0).astype(BF16)
    pieces = lax.all_to_all(jnp.broadcast_to(piece[None, None], (plane, 1, LANES)), PLANE, 0, 0, tiled=True)
    relaid = rows_in.reshape(plane, ring, 2, width).swapaxes(0, 1).reshape(balanced, width)
    gain, chol = pl.pallas_call(
        lambda *refs: select(ring, *refs),
        in_specs=[SMEM, SMEM, VMEM, VMEM, VMEM],
        out_specs=[VMEM, VMEM],
        out_shape=[
            jax.ShapeDtypeStruct((1, balanced), F32),
            jax.ShapeDtypeStruct((steps, balanced), F32),
        ],
        scratch_shapes=[pltpu.VMEM((8, width), F32)],
        name="select",
    )(
        winners,
        (me * balanced).reshape(1),
        relaid,
        pieces.reshape(plane, LANES),
        side_in[:, 1, :],
    )
    return relaid, gain.reshape(balanced), chol


def solution(mesh):
    finer = Mesh(mesh.devices.reshape(8, 4, 4, mesh.shape["grp"]), ALL)
    placed = (P(ALL, None), P(ALL), P(ALL), P(), P(ALL), P(ALL), P())
    return jax.shard_map(
        body,
        mesh=finer,
        in_specs=placed,
        out_specs=(P(ALL, None), P(ALL), P(None, ALL)),
        check_vma=False,
    )
```

```python
import jax
import jax.numpy as jnp
from jax import lax
from jax.experimental import pallas as pl
from jax.experimental.pallas import tpu as pltpu
from jax.sharding import Mesh
from jax.sharding import PartitionSpec as P

ALL = ("z", "x", "y", "core")
PLANE = ("x", "y", "core")
RING = ("x", "y", "core", "z")
RIDGE = 0.1
LANES = 128
F32 = jnp.float32
BF16 = jnp.bfloat16
VMEM = pl.BlockSpec(memory_space=pltpu.VMEM)
SMEM = pl.BlockSpec(memory_space=pltpu.SMEM)


def iota(shape, dim):
    return lax.broadcasted_iota(jnp.int32, shape, dim)


def prep(shards, plane, base, winners, counts, weight, emb, dest, quality, domain, slot_out, quality_out, win_out, picks):
    slots, width = emb.shape
    steps = winners.shape[0]
    square = (slots, slots)
    row, col = iota(square, 0), iota(square, 1)
    dest_row = dest[...].astype(F32)
    across = jnp.broadcast_to(dest_row, square)
    down = jnp.sum(jnp.where(row == col, across, 0.0), axis=1, keepdims=True)
    earlier = (down == across) & (row < col)
    rank = jnp.sum(jnp.where(earlier, 1.0, 0.0), axis=0, keepdims=True)
    lane = iota((1, slots), 1)
    valid = lane < counts[0]
    ring = shards // plane
    to = dest[...]
    to = lax.rem(to, plane) * ring + lax.div(to, plane)
    slot_out[...] = jnp.where(valid, 2 * to + rank.astype(jnp.int32), -1)
    scale = jnp.zeros((1, slots), F32)
    for k in range(weight.shape[0]):
        scale = jnp.where(domain[...] == k, weight[k], scale)
    row_quality = (quality[...] * scale).astype(BF16).astype(F32)
    quality_out[...] = row_quality

    turn = iota((8, slots), 0)
    wanted = jnp.full((8, slots), -1, jnp.int32)
    for t in range(steps):
        wanted = jnp.where(turn == t, winners[t] - base[0], wanted)
    chosen = (iota((8, slots), 1) == wanted) & valid
    spread = jnp.zeros((8, LANES), F32)
    turn_out, lane_out = iota((8, LANES), 0), iota((8, LANES), 1)
    for k, value in enumerate((row_quality, dest_row, rank)):
        mine = jnp.sum(jnp.where(chosen, value, 0.0), axis=1, keepdims=True)
        here = (lane_out == turn_out + k * steps) & (turn_out < steps)
        spread = spread + jnp.where(here, mine, 0.0)
    parts = width // LANES
    picks[...] = jnp.zeros_like(picks)
    picks[steps * parts : steps * parts + 1, :] = jnp.sum(spread, axis=0, keepdims=True)
    picked = jnp.dot(chosen.astype(F32).astype(BF16), emb[...], preferred_element_type=F32)
    for t in range(steps):
        for j in range(parts):
            picks[t * parts + j : t * parts + j + 1, :] = picked[t : t + 1, j * LANES : (j + 1) * LANES]
    win_out[...] = picks[...].astype(BF16)


def place_rows(slot, quality, emb, out):
    rows = out.shape[0]
    slots, width = emb.shape
    block = 128
    for at in range(0, rows, block):
        hit = (iota((block, slots), 0) + at) == slot[...]
        mine = jnp.sum(jnp.where(hit, quality[...], 0.0), axis=1, keepdims=True)
        hot = jnp.where(hit, 1.0, 0.0).astype(BF16)
        out[at : at + block, :width] = jnp.dot(hot, emb[...], preferred_element_type=F32).astype(BF16)
        out[at : at + block, width:] = jnp.broadcast_to(mine, (block, out.shape[1] - width)).astype(BF16)


def select(winners, base, rows, side, relaid, gain_out, chol_out, wide):
    balanced, width = relaid.shape
    steps = chol_out.shape[0]
    parts = width // LANES
    wide[...] = jnp.zeros_like(wide)
    received = side[...].astype(F32)
    for t in range(steps):
        for j in range(parts):
            wide[t : t + 1, j * LANES : (j + 1) * LANES] = received[t * parts + j : t * parts + j + 1, :]
    win = wide[...].astype(BF16)
    nt = (((1,), (1,)), ((), ()))
    relaid[...] = rows[:, :width]
    dots = lax.dot_general(win, rows[:, :width], nt, preferred_element_type=F32)
    gram = lax.dot_general(win, win, nt, preferred_element_type=F32)
    partial = jnp.zeros((balanced, LANES), F32)
    for j in range(parts):
        x = rows[:, j * LANES : (j + 1) * LANES].astype(F32)
        partial = partial + x * x
    ones = jnp.ones((8, LANES), BF16)
    norms = jnp.zeros((8, balanced), F32)
    rest = partial
    for _ in range(3):
        part = rest.astype(BF16)
        rest = rest - part.astype(F32)
        norms = norms + lax.dot_general(ones, part, nt, preferred_element_type=F32)
    norms = norms[0:1, :]
    first = jnp.where(iota((8, LANES), 1) == 0, 1.0, 0.0).astype(BF16)
    quality = lax.dot_general(first, rows[:, width:], nt, preferred_element_type=F32)[0:1, :]

    scalars = received[steps * parts : steps * parts + 1, :]
    win_quality = [scalars[:, t : 1 + t] for t in range(steps)]
    win_dest = [scalars[:, steps + t : 1 + steps + t].astype(jnp.int32) for t in range(steps)]
    win_rank = [scalars[:, 2 * steps + t : 1 + 2 * steps + t].astype(jnp.int32) for t in range(steps)]

    gain = jnp.where(quality > 0, quality * quality * norms / width + RIDGE, 0.0)
    local = iota((1, balanced), 1) + 2 * base[0]
    columns, roots, chol = [], [], []
    for t in range(steps):
        column = []
        for k in range(t):
            cross = win_quality[k] * win_quality[t] * gram[k : k + 1, t : t + 1] / width
            for e in range(k):
                cross = cross - columns[k][e] * column[e]
            column.append(cross / roots[k])
        own_gain = win_quality[t] * win_quality[t] * gram[t : t + 1, t : t + 1] / width + RIDGE
        for k in range(t):
            own_gain = own_gain - column[k] * column[k]
        root = jnp.sqrt(own_gain)
        inner = jnp.zeros((1, balanced), F32)
        for k in range(t):
            inner = inner + chol[k] * column[k]
        place = win_dest[t] * balanced + winners[t] // (balanced // 2) * 2 + win_rank[t]
        hit = jnp.where(local == place, RIDGE, 0.0)
        entry = (quality * win_quality[t] * dots[t : t + 1, :] / width + hit - inner) / root
        gain = gain - entry * entry
        columns.append(column)
        roots.append(root)
        chol.append(entry)
        chol_out[t : t + 1, :] = entry
    gain_out[...] = gain


def gathered(x, axis, rounds):
    size = lax.axis_size(axis)
    for shifts in rounds:
        came = [lax.ppermute(x, axis, [(i, (i + k) % size) for i in range(size)]) for k in shifts]
        for y in came:
            x = x + y
    return x


def body(embeds, quality, domain_ids, domain_weight, dest, counts, winners):
    shards = lax.axis_size(ALL)
    plane = lax.axis_size(PLANE)
    ring = shards // plane
    slots, width = embeds.shape
    steps = winners.shape[0]
    balanced = 2 * slots
    base = (lax.axis_index(ALL) * slots).reshape(1)
    parts = width // LANES
    held = steps * parts + 16
    small = pltpu.CompilerParams(vmem_limit_bytes=12 << 20)

    slot, row_quality, win = pl.pallas_call(
        lambda *refs: prep(shards, plane, *refs),
        in_specs=[SMEM, SMEM, SMEM, SMEM, VMEM, VMEM, VMEM, VMEM],
        out_specs=[VMEM, VMEM, VMEM],
        out_shape=[
            jax.ShapeDtypeStruct((1, slots), jnp.int32),
            jax.ShapeDtypeStruct((1, slots), F32),
            jax.ShapeDtypeStruct((held, LANES), BF16),
        ],
        scratch_shapes=[pltpu.VMEM((held, LANES), F32)],
        compiler_params=small,
        name="prep",
    )(
        base,
        winners,
        counts,
        domain_weight,
        embeds,
        dest.reshape(1, slots),
        quality.reshape(1, slots),
        domain_ids.reshape(1, slots),
    )
    win = gathered(win, "z", ((2, 4, 6), (1,)))
    send = pl.pallas_call(
        place_rows,
        in_specs=[VMEM, VMEM, VMEM],
        out_specs=VMEM,
        out_shape=jax.ShapeDtypeStruct((balanced, width + LANES), BF16),
        compiler_params=small,
        name="place_rows",
        cost_estimate=pl.CostEstimate(flops=2 * balanced * slots * width, bytes_accessed=1 << 21, transcendentals=0),
    )(slot, row_quality, embeds)
    send = send.reshape(shards, 2, width + LANES)
    rows_in = lax.all_to_all(send, RING, 0, 0, tiled=True)
    win = gathered(win, "y", ((1, 2, 3),))
    win = gathered(win, "x", ((1, 2, 3),))
    win = gathered(win, "core", ((1,),))
    rows = rows_in.reshape(plane, ring, 2, width + LANES).swapaxes(0, 1).reshape(balanced, width + LANES)
    relaid, gain, chol = pl.pallas_call(
        select,
        in_specs=[SMEM, SMEM, VMEM, VMEM],
        out_specs=[VMEM, VMEM, VMEM],
        out_shape=[
            jax.ShapeDtypeStruct((balanced, width), BF16),
            jax.ShapeDtypeStruct((1, balanced), F32),
            jax.ShapeDtypeStruct((steps, balanced), F32),
        ],
        scratch_shapes=[pltpu.VMEM((8, width), F32)],
        compiler_params=small,
        name="select",
    )(winners, base, rows, win)
    return relaid, gain.reshape(balanced), chol


def solution(mesh):
    finer = Mesh(mesh.devices.reshape(8, 4, 4, mesh.shape["grp"]), ALL)
    placed = (P(ALL, None), P(ALL), P(ALL), P(), P(ALL), P(ALL), P())
    return jax.shard_map(
        body,
        mesh=finer,
        in_specs=placed,
        out_specs=(P(ALL, None), P(ALL), P(None, ALL)),
        check_vma=False,
    )
```

```python
import jax
import jax.numpy as jnp
from jax import lax
from jax.experimental import pallas as pl
from jax.experimental.pallas import tpu as pltpu
from jax.sharding import Mesh
from jax.sharding import PartitionSpec as P

ALL = ("z", "x", "y", "core")
PLANE = ("x", "y", "core")
RIDGE = 0.1
LANES = 128
HALF = 64
F32 = jnp.float32
BF16 = jnp.bfloat16
VMEM = pl.BlockSpec(memory_space=pltpu.VMEM)
SMEM = pl.BlockSpec(memory_space=pltpu.SMEM)
HBM = pl.BlockSpec(memory_space=pltpu.HBM)


def iota(shape, dim):
    return lax.broadcasted_iota(jnp.int32, shape, dim)


def prep(base, winners, counts, weight, emb, dest, quality, domain, table_out, piece_out):
    slots, width = emb.shape
    steps = winners.shape[0]
    square = (slots, slots)
    row, col = iota(square, 0), iota(square, 1)
    dest_row = dest[...].astype(F32)
    across = jnp.broadcast_to(dest_row, square)
    down = jnp.sum(jnp.where(row == col, across, 0.0), axis=1, keepdims=True)
    earlier = (down == across) & (row < col)
    rank = jnp.sum(jnp.where(earlier, 1.0, 0.0), axis=0, keepdims=True)
    lane = iota((1, slots), 1)
    valid = lane < counts[0]
    table_out[...] = jnp.zeros_like(table_out)
    table_out[0:1, :] = jnp.where(valid, 2.0 * dest_row + rank, -1.0)
    scale = jnp.zeros((1, slots), F32)
    for k in range(weight.shape[0]):
        scale = jnp.where(domain[...] == k, weight[k], scale)
    row_quality = (quality[...] * scale).astype(BF16).astype(F32)
    table_out[1:2, :] = row_quality

    turn = iota((8, slots), 0)
    wanted = jnp.full((8, slots), -1, jnp.int32)
    for t in range(steps):
        wanted = jnp.where(turn == t, winners[t] - base[0], wanted)
    chosen = (iota((8, slots), 1) == wanted) & valid
    spread = jnp.zeros((8, LANES), F32)
    turn_out, lane_out = iota((8, LANES), 0), iota((8, LANES), 1)
    for k, value in enumerate((row_quality, dest_row, rank)):
        mine = jnp.sum(jnp.where(chosen, value, 0.0), axis=1, keepdims=True)
        here = (lane_out == turn_out + (HALF + 1 + k * steps)) & (turn_out < steps)
        spread = spread + jnp.where(here, mine, 0.0)
    table_out[2:3, :LANES] = jnp.sum(spread, axis=0, keepdims=True)
    parts = width // LANES
    picked = jnp.dot(chosen.astype(F32).astype(BF16), emb[...], preferred_element_type=F32)
    for t in range(steps):
        for j in range(parts):
            at = t * parts + j
            piece_out[at : at + 1, :] = picked[t : t + 1, j * LANES : (j + 1) * LANES]


def place_rows(table_in, pieces, emb_in, out, table, emb, sems):
    copies = (pltpu.make_async_copy(emb_in, emb, sems.at[0]), pltpu.make_async_copy(table_in, table, sems.at[1]))
    for copy in copies:
        copy.start()
    rows = out.shape[0]
    slots, width = emb.shape
    block = 128
    shape = (block, LANES)
    lane = iota(shape, 1)
    even = lax.rem(iota(shape, 0), 2) == 0
    piece = jnp.sum(pieces[...].astype(F32), axis=0, keepdims=True)
    low, high = lane < HALF, lane >= HALF
    for copy in copies:
        copy.wait()
    slot = table[0:1, :].astype(jnp.int32)
    quality = table[1:2, :]
    scalars = table[2:3, :LANES]
    fixed = jnp.where(even, jnp.where(low, piece, scalars), jnp.where(high, piece, 0.0))
    holds = lane == jnp.where(even, HALF, 0)
    for at in range(0, rows, block):
        hit = (iota((block, slots), 0) + at) == slot
        mine = jnp.sum(jnp.where(hit, quality, 0.0), axis=1, keepdims=True)
        hot = jnp.where(hit, 1.0, 0.0).astype(BF16)
        out[at : at + block, :width] = jnp.dot(hot, emb[...], preferred_element_type=F32).astype(BF16)
        out[at : at + block, width:] = jnp.where(holds, mine, fixed).astype(BF16)


def select(plane, winners, base, rows, relaid, gain_out, chol_out, wide):
    balanced, width = relaid.shape
    steps = chol_out.shape[0]
    parts = width // LANES
    nt = (((1,), (1,)), ((), ()))
    side = rows[:, width:]
    lane = iota((8, LANES), 1)
    turn = iota((8, LANES), 0)
    holds = (lane == jnp.where(turn == 0, HALF, 0)) & (turn < 2)
    both = lax.dot_general(jnp.where(holds, 1.0, 0.0).astype(BF16), side, nt, preferred_element_type=F32)
    odd = lax.rem(iota((1, balanced), 1), 2) == 1
    quality = jnp.where(odd, both[1:2, :], both[0:1, :])

    total = jnp.zeros((2 * plane, LANES), F32)
    for k in range(balanced // (2 * plane)):
        total = total + side[2 * plane * k : 2 * plane * (k + 1), :].astype(F32)
    even = lax.rem(iota((2 * plane, LANES), 0), 2) == 0
    scalars = jnp.sum(jnp.where(even, total, 0.0), axis=0, keepdims=True)
    wide[...] = jnp.zeros_like(wide)
    low = iota((1, LANES), 1) < HALF
    for t in range(steps):
        for j in range(parts):
            at = 2 * (t * parts + j)
            wide[t : t + 1, j * LANES : (j + 1) * LANES] = jnp.where(low, total[at : at + 1, :], total[at + 1 : at + 2, :])
    win = wide[...].astype(BF16)
    relaid[...] = rows[:, :width]
    dots = lax.dot_general(win, rows[:, :width], nt, preferred_element_type=F32)
    gram = lax.dot_general(win, win, nt, preferred_element_type=F32)
    partial = jnp.zeros((balanced, LANES), F32)
    for j in range(parts):
        x = rows[:, j * LANES : (j + 1) * LANES].astype(F32)
        partial = partial + x * x
    ones = jnp.ones((8, LANES), BF16)
    norms = jnp.zeros((8, balanced), F32)
    rest = partial
    for _ in range(3):
        part = rest.astype(BF16)
        rest = rest - part.astype(F32)
        norms = norms + lax.dot_general(ones, part, nt, preferred_element_type=F32)
    norms = norms[0:1, :]

    at = HALF + 1
    win_quality = [scalars[:, at + t : at + 1 + t] for t in range(steps)]
    win_dest = [scalars[:, at + steps + t : at + 1 + steps + t].astype(jnp.int32) for t in range(steps)]
    win_rank = [scalars[:, at + 2 * steps + t : at + 1 + 2 * steps + t].astype(jnp.int32) for t in range(steps)]

    gain = jnp.where(quality > 0, quality * quality * norms / width + RIDGE, 0.0)
    local = iota((1, balanced), 1) + 2 * base[0]
    columns, roots, chol = [], [], []
    for t in range(steps):
        column = []
        for k in range(t):
            cross = win_quality[k] * win_quality[t] * gram[k : k + 1, t : t + 1] / width
            for e in range(k):
                cross = cross - columns[k][e] * column[e]
            column.append(cross / roots[k])
        own_gain = win_quality[t] * win_quality[t] * gram[t : t + 1, t : t + 1] / width + RIDGE
        for k in range(t):
            own_gain = own_gain - column[k] * column[k]
        root = jnp.sqrt(own_gain)
        inner = jnp.zeros((1, balanced), F32)
        for k in range(t):
            inner = inner + chol[k] * column[k]
        place = win_dest[t] * balanced + winners[t] // (balanced // 2) * 2 + win_rank[t]
        hit = jnp.where(local == place, RIDGE, 0.0)
        entry = (quality * win_quality[t] * dots[t : t + 1, :] / width + hit - inner) / root
        gain = gain - entry * entry
        columns.append(column)
        roots.append(root)
        chol.append(entry)
        chol_out[t : t + 1, :] = entry
    gain_out[...] = gain


def body(embeds, quality, domain_ids, domain_weight, dest, counts, winners):
    shards = lax.axis_size(ALL)
    plane = lax.axis_size(PLANE)
    slots, width = embeds.shape
    steps = winners.shape[0]
    balanced = 2 * slots
    base = (lax.axis_index(ALL) * slots).reshape(1)
    small = pltpu.CompilerParams(vmem_limit_bytes=12 << 20)

    table, pieces = pl.pallas_call(
        prep,
        in_specs=[SMEM, SMEM, SMEM, SMEM, VMEM, VMEM, VMEM, VMEM],
        out_specs=[VMEM, VMEM],
        out_shape=[
            jax.ShapeDtypeStruct((8, slots), F32),
            jax.ShapeDtypeStruct((plane, LANES), F32),
        ],
        name="prep",
    )(
        base,
        winners,
        counts,
        domain_weight,
        embeds,
        dest.reshape(1, slots),
        quality.reshape(1, slots),
        domain_ids.reshape(1, slots),
    )
    pieces = pieces.astype(BF16).reshape(plane, 1, LANES)
    pieces = lax.all_to_all(pieces, PLANE, 0, 0, tiled=True).reshape(plane, LANES)
    send = pl.pallas_call(
        place_rows,
        in_specs=[HBM, VMEM, HBM],
        out_specs=VMEM,
        out_shape=jax.ShapeDtypeStruct((balanced, width + LANES), BF16),
        scratch_shapes=[
            pltpu.VMEM((8, slots), F32),
            pltpu.VMEM((slots, width), BF16),
            pltpu.SemaphoreType.DMA((2,)),
        ],
        compiler_params=small,
        name="place_rows",
    )(table, pieces, embeds)
    send = send.reshape(shards, 2, width + LANES)
    rows = lax.all_to_all(send, ALL, 0, 0, tiled=True).reshape(balanced, width + LANES)
    relaid, gain, chol = pl.pallas_call(
        lambda *refs: select(plane, *refs),
        in_specs=[SMEM, SMEM, VMEM],
        out_specs=[VMEM, VMEM, VMEM],
        out_shape=[
            jax.ShapeDtypeStruct((balanced, width), BF16),
            jax.ShapeDtypeStruct((1, balanced), F32),
            jax.ShapeDtypeStruct((steps, balanced), F32),
        ],
        scratch_shapes=[pltpu.VMEM((8, width), F32)],
        compiler_params=small,
        name="select",
    )(winners, base, rows)
    return relaid, gain.reshape(balanced), chol


def solution(mesh):
    finer = Mesh(mesh.devices.reshape(8, 4, 4, mesh.shape["grp"]), ALL)
    placed = (P(ALL, None), P(ALL), P(ALL), P(), P(ALL), P(ALL), P())
    return jax.shard_map(
        body,
        mesh=finer,
        in_specs=placed,
        out_specs=(P(ALL, None), P(ALL), P(None, ALL)),
        check_vma=False,
    )
```

```python
import jax
import jax.numpy as jnp
from jax import lax
from jax.experimental import pallas as pl
from jax.experimental.pallas import tpu as pltpu
from jax.sharding import Mesh
from jax.sharding import PartitionSpec as P

ALL = ("z", "x", "y", "core")
PLANE = ("x", "y", "core")
RIDGE = 0.1
LANES = 128
HALF = 64
F32 = jnp.float32
BF16 = jnp.bfloat16
VMEM = pl.BlockSpec(memory_space=pltpu.VMEM)
SMEM = pl.BlockSpec(memory_space=pltpu.SMEM)


def iota(shape, dim):
    return lax.broadcasted_iota(jnp.int32, shape, dim)


def place(ring, plane, base, winners, counts, weight, emb, dest, quality, domain, out, picks):
    slots, width = emb.shape
    rows = out.shape[0]
    steps = winners.shape[0]
    parts = width // LANES
    square = (slots, slots)
    row, col = iota(square, 0), iota(square, 1)
    dest_row = dest[...].astype(F32)
    across = jnp.broadcast_to(dest_row, square)
    down = jnp.sum(jnp.where(row == col, across, 0.0), axis=1, keepdims=True)
    earlier = (down == across) & (row < col)
    rank = jnp.sum(jnp.where(earlier, 1.0, 0.0), axis=0, keepdims=True)
    lane = iota((1, slots), 1)
    valid = lane < counts[0]
    here = lax.div(base[0], slots * plane)
    to = dest[...]
    offset = lax.rem(lax.div(to, plane) - here + ring, ring)
    slot = (lax.rem(to, plane) * ring + offset) * 2 + rank.astype(jnp.int32)
    slot = jnp.where(valid, slot, -1)
    scale = jnp.zeros((1, slots), F32)
    for k in range(weight.shape[0]):
        scale = jnp.where(domain[...] == k, weight[k], scale)
    row_quality = (quality[...] * scale).astype(BF16).astype(F32)

    chosen = lane == winners[0] - base[0]
    for t in range(1, steps):
        chosen = chosen | (lane == winners[t] - base[0])
    chosen = jnp.where(chosen & valid, 1.0, 0.0)
    scalars = jnp.zeros((1, LANES), F32)
    spot = iota((1, LANES), 1)
    for k, value in enumerate((row_quality, dest_row, rank)):
        mine = jnp.sum(chosen * value, axis=1, keepdims=True)
        scalars = scalars + jnp.where(spot == HALF + 1 + k, mine, 0.0)
    hot = jnp.broadcast_to(chosen, (8, slots)).astype(BF16)
    picked = jnp.dot(hot, emb[...], preferred_element_type=F32)
    for j in range(parts):
        picks[j : j + 1, :] = picked[0:1, j * LANES : (j + 1) * LANES]

    block = 128
    shape = (block, LANES)
    number = lax.rem(iota((block, parts), 0), 2 * ring)
    share = number - 2 * iota((block, parts), 1)
    share = jnp.where((share == 0) | (share == 1), 1.0, 0.0).astype(BF16)
    piece = jnp.dot(share, picks[...].astype(BF16), preferred_element_type=F32)
    spot = iota(shape, 1)
    even = lax.rem(iota(shape, 0), 2) == 0
    fixed = jnp.where(even, jnp.where(spot < HALF, piece, scalars), jnp.where(spot >= HALF, piece, 0.0))
    holds = spot == jnp.where(even, HALF, 0)
    for at in range(0, rows, block):
        hit = (iota((block, slots), 0) + at) == slot
        mine = jnp.sum(jnp.where(hit, row_quality, 0.0), axis=1, keepdims=True)
        hot = jnp.where(hit, 1.0, 0.0).astype(BF16)
        out[at : at + block, :width] = jnp.dot(hot, emb[...], preferred_element_type=F32).astype(BF16)
        out[at : at + block, width:] = jnp.where(holds, mine, fixed).astype(BF16)


def regroup(ring, plane, base, winners, rows, *outs):
    slots = rows.shape[0] // 2
    width = rows.shape[1] - LANES
    group = 2 * ring
    here = lax.div(base[0], slots * plane)
    held = []
    for t in range(winners.shape[0]):
        owner = lax.div(winners[t], slots)
        at = pl.multiple_of(lax.rem(owner, plane) * group, group)
        mine = jnp.where(lax.div(owner, plane) == here, 1.0, 0.0)
        held.append(rows[pl.ds(at, group), width:].astype(F32) * mine)
    chunk = 128
    shape = (chunk, chunk)
    to, source = iota(shape, 0), iota(shape, 1)
    per = chunk // group
    wanted = lax.rem(lax.div(to, 2), per) * group + lax.div(to, 2 * per) * 2 + lax.rem(to, 2)
    swap = jnp.where(source == wanted, 1.0, 0.0).astype(BF16)
    size = 2 * per
    spot = iota((size, LANES), 1)
    holds = spot == jnp.where(lax.rem(iota((size, LANES), 0), 2) == 0, HALF, 0)
    for c in range(rows.shape[0] // chunk):
        moved = jnp.dot(swap, rows[c * chunk : (c + 1) * chunk, :], preferred_element_type=F32)
        for k in range(ring):
            part = moved[k * size : (k + 1) * size, :]
            outs[k][c * size : (c + 1) * size, :width] = part[:, :width].astype(BF16)
            outs[k][c * size : (c + 1) * size, width:] = jnp.where(holds, part[:, width:], held[c]).astype(BF16)


def select(plane, ring, winners, base, *refs):
    blocks = refs[:ring]
    relaid, gain_out, chol_out, side, wide = refs[ring:]
    balanced, width = relaid.shape
    steps = chol_out.shape[0]
    parts = width // LANES
    nt = (((1,), (1,)), ((), ()))
    size = balanced // ring
    here = lax.div(base[0], plane * (balanced // 2))
    total = jnp.zeros((size, LANES), F32)
    for k in range(ring):
        at = pl.multiple_of(lax.rem(here - k + ring, ring) * size, size)
        relaid[pl.ds(at, size), :] = blocks[k][:, :width]
        extra = blocks[k][:, width:]
        side[pl.ds(at, size), :] = extra
        total = total + extra.astype(F32)
    lane = iota((8, LANES), 1)
    turn = iota((8, LANES), 0)
    holds = (lane == jnp.where(turn == 0, HALF, 0)) & (turn < 2)
    both = lax.dot_general(jnp.where(holds, 1.0, 0.0).astype(BF16), side[...], nt, preferred_element_type=F32)
    odd = lax.rem(iota((1, balanced), 1), 2) == 1
    quality = jnp.where(odd, both[1:2, :], both[0:1, :])

    wide[...] = jnp.zeros_like(wide)
    low = iota((1, LANES), 1) < HALF
    for t in range(steps):
        for j in range(parts):
            at = 2 * (t * parts + j)
            wide[t : t + 1, j * LANES : (j + 1) * LANES] = jnp.where(low, total[at : at + 1, :], total[at + 1 : at + 2, :])
    win = wide[...].astype(BF16)
    dots = lax.dot_general(win, relaid[...], nt, preferred_element_type=F32)
    gram = lax.dot_general(win, win, nt, preferred_element_type=F32)
    partial = jnp.zeros((balanced, LANES), F32)
    for j in range(parts):
        x = relaid[:, j * LANES : (j + 1) * LANES].astype(F32)
        partial = partial + x * x
    ones = jnp.ones((8, LANES), BF16)
    norms = jnp.zeros((8, balanced), F32)
    rest = partial
    for _ in range(3):
        part = rest.astype(BF16)
        rest = rest - part.astype(F32)
        norms = norms + lax.dot_general(ones, part, nt, preferred_element_type=F32)
    norms = norms[0:1, :]

    def scalar(t, k):
        at = 2 * t * parts
        return total[at : at + 1, HALF + 1 + k : HALF + 2 + k]

    win_quality = [scalar(t, 0) for t in range(steps)]
    win_dest = [scalar(t, 1).astype(jnp.int32) for t in range(steps)]
    win_rank = [scalar(t, 2).astype(jnp.int32) for t in range(steps)]

    gain = jnp.where(quality > 0, quality * quality * norms / width + RIDGE, 0.0)
    local = iota((1, balanced), 1) + 2 * base[0]
    columns, roots, chol = [], [], []
    for t in range(steps):
        column = []
        for k in range(t):
            cross = win_quality[k] * win_quality[t] * gram[k : k + 1, t : t + 1] / width
            for e in range(k):
                cross = cross - columns[k][e] * column[e]
            column.append(cross / roots[k])
        own_gain = win_quality[t] * win_quality[t] * gram[t : t + 1, t : t + 1] / width + RIDGE
        for k in range(t):
            own_gain = own_gain - column[k] * column[k]
        root = jnp.sqrt(own_gain)
        inner = jnp.zeros((1, balanced), F32)
        for k in range(t):
            inner = inner + chol[k] * column[k]
        place = win_dest[t] * balanced + winners[t] // (balanced // 2) * 2 + win_rank[t]
        hit = jnp.where(local == place, RIDGE, 0.0)
        entry = (quality * win_quality[t] * dots[t : t + 1, :] / width + hit - inner) / root
        gain = gain - entry * entry
        columns.append(column)
        roots.append(root)
        chol.append(entry)
        chol_out[t : t + 1, :] = entry
    gain_out[...] = gain


def body(embeds, quality, domain_ids, domain_weight, dest, counts, winners):
    plane = lax.axis_size(PLANE)
    ring = lax.axis_size("z")
    slots, width = embeds.shape
    steps = winners.shape[0]
    balanced = 2 * slots
    base = (lax.axis_index(ALL) * slots).reshape(1)
    small = pltpu.CompilerParams(vmem_limit_bytes=12 << 20)
    broad = width + LANES
    size = balanced // ring

    send = pl.pallas_call(
        lambda *refs: place(ring, plane, *refs),
        in_specs=[SMEM, SMEM, SMEM, SMEM, VMEM, VMEM, VMEM, VMEM],
        out_specs=VMEM,
        out_shape=jax.ShapeDtypeStruct((balanced, broad), BF16),
        scratch_shapes=[pltpu.VMEM((width // LANES, LANES), F32)],
        name="place",
    )(
        base,
        winners,
        counts,
        domain_weight,
        embeds,
        dest.reshape(1, slots),
        quality.reshape(1, slots),
        domain_ids.reshape(1, slots),
    )
    rows = lax.all_to_all(send.reshape(plane, 2 * ring, broad), PLANE, 0, 0, tiled=True)
    blocks = pl.pallas_call(
        lambda *refs: regroup(ring, plane, *refs),
        in_specs=[SMEM, SMEM, VMEM],
        out_specs=[VMEM] * ring,
        out_shape=[jax.ShapeDtypeStruct((size, broad), BF16)] * ring,
        compiler_params=small,
        name="regroup",
    )(base, winners, rows.reshape(balanced, broad))
    came = list(blocks)
    for k in (4, 3, 5, 2, 6, 1, 7):
        came[k] = lax.ppermute(blocks[k], "z", [(i, (i + k) % ring) for i in range(ring)])
    relaid, gain, chol = pl.pallas_call(
        lambda *refs: select(plane, ring, *refs),
        in_specs=[SMEM, SMEM] + [VMEM] * ring,
        out_specs=[VMEM, VMEM, VMEM],
        out_shape=[
            jax.ShapeDtypeStruct((balanced, width), BF16),
            jax.ShapeDtypeStruct((1, balanced), F32),
            jax.ShapeDtypeStruct((steps, balanced), F32),
        ],
        scratch_shapes=[pltpu.VMEM((balanced, LANES), BF16), pltpu.VMEM((8, width), F32)],
        compiler_params=small,
        name="select",
    )(winners, base, *came)
    return relaid, gain.reshape(balanced), chol


def solution(mesh):
    finer = Mesh(mesh.devices.reshape(8, 4, 4, mesh.shape["grp"]), ALL)
    placed = (P(ALL, None), P(ALL), P(ALL), P(), P(ALL), P(ALL), P())
    return jax.shard_map(
        body,
        mesh=finer,
        in_specs=placed,
        out_specs=(P(ALL, None), P(ALL), P(None, ALL)),
        check_vma=False,
    )
```

```python
import jax
import jax.numpy as jnp
from jax import lax
from jax.experimental import pallas as pl
from jax.experimental.pallas import tpu as pltpu
from jax.sharding import Mesh
from jax.sharding import PartitionSpec as P

ALL = ("z", "x", "y", "core")
RIDGE = 0.1
LANES = 128
F32 = jnp.float32
BF16 = jnp.bfloat16
VMEM = pl.BlockSpec(memory_space=pltpu.VMEM)
SMEM = pl.BlockSpec(memory_space=pltpu.SMEM)


def iota(shape, dim):
    return lax.broadcasted_iota(jnp.int32, shape, dim)


def place(base, winners, counts, weight, emb, dest, quality, domain, out, win_out, picks):
    slots, width = emb.shape
    rows = out.shape[0]
    steps = winners.shape[0]
    parts = width // LANES
    square = (slots, slots)
    row, col = iota(square, 0), iota(square, 1)
    dest_row = dest[...].astype(F32)
    across = jnp.broadcast_to(dest_row, square)
    down = jnp.sum(jnp.where(row == col, across, 0.0), axis=1, keepdims=True)
    earlier = (down == across) & (row < col)
    rank = jnp.sum(jnp.where(earlier, 1.0, 0.0), axis=0, keepdims=True)
    lane = iota((1, slots), 1)
    valid = lane < counts[0]
    slot = jnp.where(valid, 2 * dest[...] + rank.astype(jnp.int32), -1)
    scale = jnp.zeros((1, slots), F32)
    for k in range(weight.shape[0]):
        scale = jnp.where(domain[...] == k, weight[k], scale)
    row_quality = (quality[...] * scale).astype(BF16).astype(F32)

    turn = iota((8, slots), 0)
    wanted = jnp.full((8, slots), -1, jnp.int32)
    for t in range(steps):
        wanted = jnp.where(turn == t, winners[t] - base[0], wanted)
    chosen = (iota((8, slots), 1) == wanted) & valid
    spread = jnp.zeros((8, LANES), F32)
    turn_out, lane_out = iota((8, LANES), 0), iota((8, LANES), 1)
    for k, value in enumerate((row_quality, dest_row, rank)):
        mine = jnp.sum(jnp.where(chosen, value, 0.0), axis=1, keepdims=True)
        here = (lane_out == turn_out + k * steps) & (turn_out < steps)
        spread = spread + jnp.where(here, mine, 0.0)
    picks[...] = jnp.zeros_like(picks)
    picks[steps * parts : steps * parts + 1, :] = jnp.sum(spread, axis=0, keepdims=True)
    picked = jnp.dot(chosen.astype(F32).astype(BF16), emb[...], preferred_element_type=F32)
    for t in range(steps):
        for j in range(parts):
            picks[t * parts + j : t * parts + j + 1, :] = picked[t : t + 1, j * LANES : (j + 1) * LANES]
    win_out[...] = picks[...].astype(BF16)

    block = 128
    for at in range(0, rows, block):
        hit = (iota((block, slots), 0) + at) == slot
        mine = jnp.sum(jnp.where(hit, row_quality, 0.0), axis=1, keepdims=True)
        hot = jnp.where(hit, 1.0, 0.0).astype(BF16)
        out[at : at + block, :width] = jnp.dot(hot, emb[...], preferred_element_type=F32).astype(BF16)
        out[at : at + block, width:] = jnp.broadcast_to(mine, (block, out.shape[1] - width)).astype(BF16)


def select(winners, base, rows, side, relaid, gain_out, chol_out, wide):
    balanced, width = relaid.shape
    steps = chol_out.shape[0]
    parts = width // LANES
    wide[...] = jnp.zeros_like(wide)
    received = side[...].astype(F32)
    for t in range(steps):
        for j in range(parts):
            wide[t : t + 1, j * LANES : (j + 1) * LANES] = received[t * parts + j : t * parts + j + 1, :]
    win = wide[...].astype(BF16)
    nt = (((1,), (1,)), ((), ()))
    relaid[...] = rows[:, :width]
    dots = lax.dot_general(win, rows[:, :width], nt, preferred_element_type=F32)
    gram = lax.dot_general(win, win, nt, preferred_element_type=F32)
    partial = jnp.zeros((balanced, LANES), F32)
    for j in range(parts):
        x = rows[:, j * LANES : (j + 1) * LANES].astype(F32)
        partial = partial + x * x
    ones = jnp.ones((8, LANES), BF16)
    norms = jnp.zeros((8, balanced), F32)
    rest = partial
    for _ in range(3):
        part = rest.astype(BF16)
        rest = rest - part.astype(F32)
        norms = norms + lax.dot_general(ones, part, nt, preferred_element_type=F32)
    norms = norms[0:1, :]
    first = jnp.where(iota((8, LANES), 1) == 0, 1.0, 0.0).astype(BF16)
    quality = lax.dot_general(first, rows[:, width:], nt, preferred_element_type=F32)[0:1, :]

    scalars = received[steps * parts : steps * parts + 1, :]
    win_quality = [scalars[:, t : 1 + t] for t in range(steps)]
    win_dest = [scalars[:, steps + t : 1 + steps + t].astype(jnp.int32) for t in range(steps)]
    win_rank = [scalars[:, 2 * steps + t : 1 + 2 * steps + t].astype(jnp.int32) for t in range(steps)]

    gain = jnp.where(quality > 0, quality * quality * norms / width + RIDGE, 0.0)
    local = iota((1, balanced), 1) + 2 * base[0]
    columns, roots, chol = [], [], []
    for t in range(steps):
        column = []
        for k in range(t):
            cross = win_quality[k] * win_quality[t] * gram[k : k + 1, t : t + 1] / width
            for e in range(k):
                cross = cross - columns[k][e] * column[e]
            column.append(cross / roots[k])
        own_gain = win_quality[t] * win_quality[t] * gram[t : t + 1, t : t + 1] / width + RIDGE
        for k in range(t):
            own_gain = own_gain - column[k] * column[k]
        root = jnp.sqrt(own_gain)
        inner = jnp.zeros((1, balanced), F32)
        for k in range(t):
            inner = inner + chol[k] * column[k]
        place = win_dest[t] * balanced + winners[t] // (balanced // 2) * 2 + win_rank[t]
        hit = jnp.where(local == place, RIDGE, 0.0)
        entry = (quality * win_quality[t] * dots[t : t + 1, :] / width + hit - inner) / root
        gain = gain - entry * entry
        columns.append(column)
        roots.append(root)
        chol.append(entry)
        chol_out[t : t + 1, :] = entry
    gain_out[...] = gain


def gathered(x, axis, rounds):
    size = lax.axis_size(axis)
    for shifts in rounds:
        came = [lax.ppermute(x, axis, [(i, (i + k) % size) for i in range(size)]) for k in shifts]
        for y in came:
            x = x + y
    return x


def body(embeds, quality, domain_ids, domain_weight, dest, counts, winners):
    shards = lax.axis_size(ALL)
    slots, width = embeds.shape
    steps = winners.shape[0]
    balanced = 2 * slots
    base = (lax.axis_index(ALL) * slots).reshape(1)
    broad = width + LANES
    held = steps * (width // LANES) + 8

    send, win = pl.pallas_call(
        place,
        in_specs=[SMEM, SMEM, SMEM, SMEM, VMEM, VMEM, VMEM, VMEM],
        out_specs=[VMEM, VMEM],
        out_shape=[
            jax.ShapeDtypeStruct((balanced, broad), BF16),
            jax.ShapeDtypeStruct((held, LANES), BF16),
        ],
        scratch_shapes=[pltpu.VMEM((held, LANES), F32)],
        name="place",
    )(
        base,
        winners,
        counts,
        domain_weight,
        embeds,
        dest.reshape(1, slots),
        quality.reshape(1, slots),
        domain_ids.reshape(1, slots),
    )
    rows = lax.all_to_all(send.reshape(shards, 2, broad), ALL, 0, 0, tiled=True).reshape(balanced, broad)
    win = gathered(win, "core", ((1,),))
    win = gathered(win, "y", ((1, 2, 3),))
    win = gathered(win, "x", ((1, 2, 3),))
    win = gathered(win, "z", ((2, 4, 6), (1,)))
    relaid, gain, chol = pl.pallas_call(
        select,
        in_specs=[SMEM, SMEM, VMEM, VMEM],
        out_specs=[VMEM, VMEM, VMEM],
        out_shape=[
            jax.ShapeDtypeStruct((balanced, width), BF16),
            jax.ShapeDtypeStruct((1, balanced), F32),
            jax.ShapeDtypeStruct((steps, balanced), F32),
        ],
        scratch_shapes=[pltpu.VMEM((8, width), F32)],
        compiler_params=pltpu.CompilerParams(vmem_limit_bytes=12 << 20),
        name="select",
    )(winners, base, rows, win)
    return relaid, gain.reshape(balanced), chol


def solution(mesh):
    finer = Mesh(mesh.devices.reshape(8, 4, 4, mesh.shape["grp"]), ALL)
    placed = (P(ALL, None), P(ALL), P(ALL), P(), P(ALL), P(ALL), P())
    return jax.shard_map(
        body,
        mesh=finer,
        in_specs=placed,
        out_specs=(P(ALL, None), P(ALL), P(None, ALL)),
        check_vma=False,
    )
```

```python
import jax
import jax.numpy as jnp
from jax import lax
from jax.experimental import pallas as pl
from jax.experimental.pallas import tpu as pltpu
from jax.sharding import Mesh
from jax.sharding import PartitionSpec as P

ALL = ("z", "x", "y", "core")
RIDGE = 0.1
LANES = 128
F32 = jnp.float32
BF16 = jnp.bfloat16
VMEM = pl.BlockSpec(memory_space=pltpu.VMEM)
SMEM = pl.BlockSpec(memory_space=pltpu.SMEM)


def iota(shape, dim):
    return lax.broadcasted_iota(jnp.int32, shape, dim)


def place(base, winners, counts, weight, emb, dest, quality, domain, out, win_out, picks):
    slots, width = emb.shape
    rows = 2 * out.shape[0]
    steps = winners.shape[0]
    parts = width // LANES
    square = (slots, slots)
    row, col = iota(square, 0), iota(square, 1)
    dest_row = dest[...].astype(F32)
    across = jnp.broadcast_to(dest_row, square)
    down = jnp.sum(jnp.where(row == col, across, 0.0), axis=1, keepdims=True)
    earlier = (down == across) & (row < col)
    rank = jnp.sum(jnp.where(earlier, 1.0, 0.0), axis=0, keepdims=True)
    lane = iota((1, slots), 1)
    valid = lane < counts[0]
    slot = jnp.where(valid, 2 * dest[...] + rank.astype(jnp.int32), -1)
    scale = jnp.zeros((1, slots), F32)
    for k in range(weight.shape[0]):
        scale = jnp.where(domain[...] == k, weight[k], scale)
    row_quality = (quality[...] * scale).astype(BF16).astype(F32)

    turn = iota((8, slots), 0)
    wanted = jnp.full((8, slots), -1, jnp.int32)
    for t in range(steps):
        wanted = jnp.where(turn == t, winners[t] - base[0], wanted)
    chosen = (iota((8, slots), 1) == wanted) & valid
    spread = jnp.zeros((8, LANES), F32)
    turn_out, lane_out = iota((8, LANES), 0), iota((8, LANES), 1)
    for k, value in enumerate((row_quality, dest_row, rank)):
        mine = jnp.sum(jnp.where(chosen, value, 0.0), axis=1, keepdims=True)
        here = (lane_out == turn_out + k * steps) & (turn_out < steps)
        spread = spread + jnp.where(here, mine, 0.0)
    picks[...] = jnp.zeros_like(picks)
    picks[steps * parts : steps * parts + 1, :] = jnp.sum(spread, axis=0, keepdims=True)
    picked = jnp.dot(chosen.astype(F32).astype(BF16), emb[...], preferred_element_type=F32)
    for t in range(steps):
        for j in range(parts):
            picks[t * parts + j : t * parts + j + 1, :] = picked[t : t + 1, j * LANES : (j + 1) * LANES]
    win_out[...] = picks[...].astype(BF16)

    block = 128
    for at in range(0, rows, block):
        hit = (iota((block, slots), 0) + at) == slot
        mine = jnp.sum(jnp.where(hit, row_quality, 0.0), axis=1, keepdims=True)
        hot = jnp.where(hit, 1.0, 0.0).astype(BF16)
        pair = slice(at // 2, (at + block) // 2)
        moved = jnp.dot(hot, emb[...], preferred_element_type=F32).astype(BF16)
        out[pair, :, :width] = moved.reshape(block // 2, 2, width)
        mine = jnp.broadcast_to(mine, (block, LANES)).astype(BF16)
        out[pair, :, width:] = mine.reshape(block // 2, 2, LANES)


def select(winners, base, rows, side, relaid, gain_out, chol_out, wide, sem):
    balanced, width = relaid.shape
    copy = pltpu.make_async_copy(rows.at[:, pl.ds(0, width)], relaid, sem)
    copy.start()
    steps = chol_out.shape[0]
    parts = width // LANES
    wide[...] = jnp.zeros_like(wide)
    received = side[...].astype(F32)
    for t in range(steps):
        for j in range(parts):
            wide[t : t + 1, j * LANES : (j + 1) * LANES] = received[t * parts + j : t * parts + j + 1, :]
    win = wide[...].astype(BF16)
    nt = (((1,), (1,)), ((), ()))
    dots = lax.dot_general(win, rows[:, :width], nt, preferred_element_type=F32)
    gram = lax.dot_general(win, win, nt, preferred_element_type=F32)
    partial = jnp.zeros((balanced, LANES), F32)
    for j in range(parts):
        x = rows[:, j * LANES : (j + 1) * LANES].astype(F32)
        partial = partial + x * x
    ones = jnp.ones((8, LANES), BF16)
    norms = jnp.zeros((8, balanced), F32)
    rest = partial
    for _ in range(3):
        part = rest.astype(BF16)
        rest = rest - part.astype(F32)
        norms = norms + lax.dot_general(ones, part, nt, preferred_element_type=F32)
    norms = norms[0:1, :]
    first = jnp.where(iota((8, LANES), 1) == 0, 1.0, 0.0).astype(BF16)
    quality = lax.dot_general(first, rows[:, width:], nt, preferred_element_type=F32)[0:1, :]

    scalars = received[steps * parts : steps * parts + 1, :]
    win_quality = [scalars[:, t : 1 + t] for t in range(steps)]
    win_dest = [scalars[:, steps + t : 1 + steps + t].astype(jnp.int32) for t in range(steps)]
    win_rank = [scalars[:, 2 * steps + t : 1 + 2 * steps + t].astype(jnp.int32) for t in range(steps)]

    gain = jnp.where(quality > 0, quality * quality * norms / width + RIDGE, 0.0)
    local = iota((1, balanced), 1) + 2 * base[0]
    columns, roots, chol = [], [], []
    for t in range(steps):
        column = []
        for k in range(t):
            cross = win_quality[k] * win_quality[t] * gram[k : k + 1, t : t + 1] / width
            for e in range(k):
                cross = cross - columns[k][e] * column[e]
            column.append(cross / roots[k])
        own_gain = win_quality[t] * win_quality[t] * gram[t : t + 1, t : t + 1] / width + RIDGE
        for k in range(t):
            own_gain = own_gain - column[k] * column[k]
        root = jnp.sqrt(own_gain)
        inner = jnp.zeros((1, balanced), F32)
        for k in range(t):
            inner = inner + chol[k] * column[k]
        place = win_dest[t] * balanced + winners[t] // (balanced // 2) * 2 + win_rank[t]
        hit = jnp.where(local == place, RIDGE, 0.0)
        entry = (quality * win_quality[t] * dots[t : t + 1, :] / width + hit - inner) / root
        gain = gain - entry * entry
        columns.append(column)
        roots.append(root)
        chol.append(entry)
        chol_out[t : t + 1, :] = entry
    gain_out[...] = gain
    copy.wait()


def gathered(x, axis, rounds):
    size = lax.axis_size(axis)
    for shifts in rounds:
        came = [lax.ppermute(x, axis, [(i, (i + k) % size) for i in range(size)]) for k in shifts]
        for y in came:
            x = x + y
    return x


def body(embeds, quality, domain_ids, domain_weight, dest, counts, winners):
    shards = lax.axis_size(ALL)
    slots, width = embeds.shape
    steps = winners.shape[0]
    balanced = 2 * slots
    base = (lax.axis_index(ALL) * slots).reshape(1)
    broad = width + LANES
    held = steps * (width // LANES) + 8

    send, win = pl.pallas_call(
        place,
        in_specs=[SMEM, SMEM, SMEM, SMEM, VMEM, VMEM, VMEM, VMEM],
        out_specs=[VMEM, VMEM],
        out_shape=[
            jax.ShapeDtypeStruct((shards, 2, broad), BF16),
            jax.ShapeDtypeStruct((held, LANES), BF16),
        ],
        scratch_shapes=[pltpu.VMEM((held, LANES), F32)],

        name="place",
    )(
        base,
        winners,
        counts,
        domain_weight,
        embeds,
        dest.reshape(1, slots),
        quality.reshape(1, slots),
        domain_ids.reshape(1, slots),
    )
    rows = lax.all_to_all(send, ALL, 0, 0, tiled=True).reshape(balanced, broad)
    win = gathered(win, "core", ((1,),))
    win = gathered(win, "y", ((1, 2, 3),))
    win = gathered(win, "x", ((1, 2, 3),))
    win = gathered(win, "z", ((4, 3, 5, 2, 6, 1, 7),))
    relaid, gain, chol = pl.pallas_call(
        select,
        in_specs=[SMEM, SMEM, VMEM, VMEM],
        out_specs=[pl.BlockSpec(memory_space=pl.ANY), VMEM, VMEM],
        out_shape=[
            jax.ShapeDtypeStruct((balanced, width), BF16),
            jax.ShapeDtypeStruct((1, balanced), F32),
            jax.ShapeDtypeStruct((steps, balanced), F32),
        ],
        scratch_shapes=[pltpu.VMEM((8, width), F32), pltpu.SemaphoreType.DMA],
        compiler_params=pltpu.CompilerParams(vmem_limit_bytes=12 << 20),
        name="select",
    )(winners, base, rows, win)
    return relaid, gain.reshape(balanced), chol


def solution(mesh):
    finer = Mesh(mesh.devices.reshape(8, 4, 4, mesh.shape["grp"]), ALL)
    placed = (P(ALL, None), P(ALL), P(ALL), P(), P(ALL), P(ALL), P())
    return jax.shard_map(
        body,
        mesh=finer,
        in_specs=placed,
        out_specs=(P(ALL, None), P(ALL), P(None, ALL)),
        check_vma=False,
    )
```

```python
import jax
import jax.numpy as jnp
from jax import lax
from jax.experimental import pallas as pl
from jax.experimental.pallas import tpu as pltpu
from jax.sharding import Mesh
from jax.sharding import PartitionSpec as P

ALL = ("z", "x", "y", "core")
RIDGE = 0.1
LANES = 128
F32 = jnp.float32
BF16 = jnp.bfloat16
VMEM = pl.BlockSpec(memory_space=pltpu.VMEM)
SMEM = pl.BlockSpec(memory_space=pltpu.SMEM)


def iota(shape, dim):
    return lax.broadcasted_iota(jnp.int32, shape, dim)


def place(base, winners, counts, weight, emb, dest, quality, domain, out, win_out, picks):
    slots, width = emb.shape
    rows = 2 * out.shape[0]
    steps = winners.shape[0]
    parts = width // LANES
    square = (slots, slots)
    row, col = iota(square, 0), iota(square, 1)
    dest_row = dest[...].astype(F32)
    across = jnp.broadcast_to(dest_row, square)
    down = jnp.sum(jnp.where(row == col, across, 0.0), axis=1, keepdims=True)
    earlier = (down == across) & (row < col)
    rank = jnp.sum(jnp.where(earlier, 1.0, 0.0), axis=0, keepdims=True)
    lane = iota((1, slots), 1)
    valid = lane < counts[0]
    slot = jnp.where(valid, 2 * dest[...] + rank.astype(jnp.int32), -1)
    scale = jnp.zeros((1, slots), F32)
    for k in range(weight.shape[0]):
        scale = jnp.where(domain[...] == k, weight[k], scale)
    row_quality = (quality[...] * scale).astype(BF16).astype(F32)

    turn = iota((8, slots), 0)
    wanted = jnp.full((8, slots), -1, jnp.int32)
    for t in range(steps):
        wanted = jnp.where(turn == t, winners[t] - base[0], wanted)
    chosen = (iota((8, slots), 1) == wanted) & valid
    spread = jnp.zeros((8, LANES), F32)
    turn_out, lane_out = iota((8, LANES), 0), iota((8, LANES), 1)
    for k, value in enumerate((row_quality, dest_row, rank)):
        mine = jnp.sum(jnp.where(chosen, value, 0.0), axis=1, keepdims=True)
        here = (lane_out == turn_out + k * steps) & (turn_out < steps)
        spread = spread + jnp.where(here, mine, 0.0)
    picks[...] = jnp.zeros_like(picks)
    picks[steps * parts : steps * parts + 1, :] = jnp.sum(spread, axis=0, keepdims=True)
    picked = jnp.dot(chosen.astype(F32).astype(BF16), emb[...], preferred_element_type=F32)
    for t in range(steps):
        for j in range(parts):
            picks[t * parts + j : t * parts + j + 1, :] = picked[t : t + 1, j * LANES : (j + 1) * LANES]
    win_out[...] = picks[...].astype(BF16)

    block = 128
    for at in range(0, rows, block):
        hit = (iota((block, slots), 0) + at) == slot
        mine = jnp.sum(jnp.where(hit, row_quality, 0.0), axis=1, keepdims=True)
        hot = jnp.where(hit, 1.0, 0.0).astype(BF16)
        pair = slice(at // 2, (at + block) // 2)
        moved = jnp.dot(hot, emb[...], preferred_element_type=F32).astype(BF16)
        out[pair, :, :width] = moved.reshape(block // 2, 2, width)
        mine = jnp.broadcast_to(mine, (block, LANES)).astype(BF16)
        out[pair, :, width:] = mine.reshape(block // 2, 2, LANES)


def select(winners, base, rows, side, relaid, gain_out, chol_out, wide, extra):
    balanced, width = relaid.shape
    steps = chol_out.shape[0]
    parts = width // LANES
    wide[...] = jnp.zeros_like(wide)
    received = side[...].astype(F32)
    for t in range(steps):
        for j in range(parts):
            wide[t : t + 1, j * LANES : (j + 1) * LANES] = received[t * parts + j : t * parts + j + 1, :]
    win = wide[...].astype(BF16)
    nt = (((1,), (1,)), ((), ()))
    block = 128
    for at in range(0, balanced, block):
        moved = rows[at // 2 : (at + block) // 2].reshape(block, width + LANES)
        relaid[at : at + block, :] = moved[:, :width]
        extra[at : at + block, :] = moved[:, width:]
    dots = lax.dot_general(win, relaid[...], nt, preferred_element_type=F32)
    gram = lax.dot_general(win, win, nt, preferred_element_type=F32)
    partial = jnp.zeros((balanced, LANES), F32)
    for j in range(parts):
        x = relaid[:, j * LANES : (j + 1) * LANES].astype(F32)
        partial = partial + x * x
    ones = jnp.ones((8, LANES), BF16)
    norms = jnp.zeros((8, balanced), F32)
    rest = partial
    for _ in range(3):
        part = rest.astype(BF16)
        rest = rest - part.astype(F32)
        norms = norms + lax.dot_general(ones, part, nt, preferred_element_type=F32)
    norms = norms[0:1, :]
    first = jnp.where(iota((8, LANES), 1) == 0, 1.0, 0.0).astype(BF16)
    quality = lax.dot_general(first, extra[...], nt, preferred_element_type=F32)[0:1, :]

    scalars = received[steps * parts : steps * parts + 1, :]
    win_quality = [scalars[:, t : 1 + t] for t in range(steps)]
    win_dest = [scalars[:, steps + t : 1 + steps + t].astype(jnp.int32) for t in range(steps)]
    win_rank = [scalars[:, 2 * steps + t : 1 + 2 * steps + t].astype(jnp.int32) for t in range(steps)]

    gain = jnp.where(quality > 0, quality * quality * norms / width + RIDGE, 0.0)
    local = iota((1, balanced), 1) + 2 * base[0]
    columns, roots, chol = [], [], []
    for t in range(steps):
        column = []
        for k in range(t):
            cross = win_quality[k] * win_quality[t] * gram[k : k + 1, t : t + 1] / width
            for e in range(k):
                cross = cross - columns[k][e] * column[e]
            column.append(cross / roots[k])
        own_gain = win_quality[t] * win_quality[t] * gram[t : t + 1, t : t + 1] / width + RIDGE
        for k in range(t):
            own_gain = own_gain - column[k] * column[k]
        root = jnp.sqrt(own_gain)
        inner = jnp.zeros((1, balanced), F32)
        for k in range(t):
            inner = inner + chol[k] * column[k]
        place = win_dest[t] * balanced + winners[t] // (balanced // 2) * 2 + win_rank[t]
        hit = jnp.where(local == place, RIDGE, 0.0)
        entry = (quality * win_quality[t] * dots[t : t + 1, :] / width + hit - inner) / root
        gain = gain - entry * entry
        columns.append(column)
        roots.append(root)
        chol.append(entry)
        chol_out[t : t + 1, :] = entry
    gain_out[...] = gain


def gathered(x, axis, rounds):
    size = lax.axis_size(axis)
    for shifts in rounds:
        came = [lax.ppermute(x, axis, [(i, (i + k) % size) for i in range(size)]) for k in shifts]
        for y in came:
            x = x + y
    return x


def along_ring(x):
    ring = lax.axis_size("z")
    total = None
    for k in range(1, ring // 2 + 1):
        back = k % (ring // 2)
        moves = []
        for i in range(ring):
            moves.append((2 * i, 2 * ((i + k) % ring)))
            moves.append((2 * i + 1, 2 * ((i - back) % ring) + 1))
        came = lax.ppermute(x, ("z", "core"), moves)
        total = came if total is None else total + came
    return total


def body(embeds, quality, domain_ids, domain_weight, dest, counts, winners):
    shards = lax.axis_size(ALL)
    slots, width = embeds.shape
    steps = winners.shape[0]
    balanced = 2 * slots
    base = (lax.axis_index(ALL) * slots).reshape(1)
    broad = width + LANES
    held = steps * (width // LANES) + 8

    send, win = pl.pallas_call(
        place,
        in_specs=[SMEM, SMEM, SMEM, SMEM, VMEM, VMEM, VMEM, VMEM],
        out_specs=[VMEM, VMEM],
        out_shape=[
            jax.ShapeDtypeStruct((shards, 2, broad), BF16),
            jax.ShapeDtypeStruct((held, LANES), BF16),
        ],
        scratch_shapes=[pltpu.VMEM((held, LANES), F32)],

        name="place",
    )(
        base,
        winners,
        counts,
        domain_weight,
        embeds,
        dest.reshape(1, slots),
        quality.reshape(1, slots),
        domain_ids.reshape(1, slots),
    )
    rows = lax.all_to_all(send, ALL, 0, 0, tiled=True)
    win = gathered(win, "core", ((1,),))
    win = gathered(win, "y", ((1, 2, 3),))
    win = gathered(win, "x", ((1, 2, 3),))
    win = gathered(along_ring(win), "core", ((1,),))
    relaid, gain, chol = pl.pallas_call(
        select,
        in_specs=[SMEM, SMEM, VMEM, VMEM],
        out_specs=[VMEM, VMEM, VMEM],
        out_shape=[
            jax.ShapeDtypeStruct((balanced, width), BF16),
            jax.ShapeDtypeStruct((1, balanced), F32),
            jax.ShapeDtypeStruct((steps, balanced), F32),
        ],
        scratch_shapes=[pltpu.VMEM((8, width), F32), pltpu.VMEM((balanced, LANES), BF16)],
        compiler_params=pltpu.CompilerParams(vmem_limit_bytes=12 << 20),
        name="select",
    )(winners, base, rows, win)
    return relaid, gain.reshape(balanced), chol


def solution(mesh):
    finer = Mesh(mesh.devices.reshape(8, 4, 4, mesh.shape["grp"]), ALL)
    placed = (P(ALL, None), P(ALL), P(ALL), P(), P(ALL), P(ALL), P())
    return jax.shard_map(
        body,
        mesh=finer,
        in_specs=placed,
        out_specs=(P(ALL, None), P(ALL), P(None, ALL)),
        check_vma=False,
    )
```

```python
import jax
import jax.numpy as jnp
from jax import lax
from jax.experimental import pallas as pl
from jax.experimental.pallas import tpu as pltpu
from jax.sharding import Mesh
from jax.sharding import PartitionSpec as P


ALL = ("z", "x", "y", "core")
RIDGE = 0.1
LANES = 128
F32 = jnp.float32
BF16 = jnp.bfloat16
VMEM = pl.BlockSpec(memory_space=pltpu.VMEM)
SMEM = pl.BlockSpec(memory_space=pltpu.SMEM)


def iota(shape, dim):
    return lax.broadcasted_iota(jnp.int32, shape, dim)


def place(base, winners, counts, weight, emb, dest, quality, domain, out, win_out, picks):
    slots, width = emb.shape
    rows = 2 * out.shape[0]
    steps = winners.shape[0]
    parts = width // LANES
    square = (slots, slots)
    row, col = iota(square, 0), iota(square, 1)
    dest_row = dest[...].astype(F32)
    across = jnp.broadcast_to(dest_row, square)
    down = jnp.sum(jnp.where(row == col, across, 0.0), axis=1, keepdims=True)
    earlier = (down == across) & (row < col)
    rank = jnp.sum(jnp.where(earlier, 1.0, 0.0), axis=0, keepdims=True)
    lane = iota((1, slots), 1)
    valid = lane < counts[0]
    slot = jnp.where(valid, 2 * dest[...] + rank.astype(jnp.int32), -1)
    scale = jnp.zeros((1, slots), F32)
    for k in range(weight.shape[0]):
        scale = jnp.where(domain[...] == k, weight[k], scale)
    row_quality = (quality[...] * scale).astype(BF16).astype(F32)

    turn = iota((8, slots), 0)
    wanted = jnp.full((8, slots), -1, jnp.int32)
    for t in range(steps):
        wanted = jnp.where(turn == t, winners[t] - base[0], wanted)
    chosen = (iota((8, slots), 1) == wanted) & valid
    spread = jnp.zeros((8, LANES), F32)
    turn_out, lane_out = iota((8, LANES), 0), iota((8, LANES), 1)
    for k, value in enumerate((row_quality, dest_row, rank)):
        mine = jnp.sum(jnp.where(chosen, value, 0.0), axis=1, keepdims=True)
        here = (lane_out == turn_out + k * steps) & (turn_out < steps)
        spread = spread + jnp.where(here, mine, 0.0)
    picks[...] = jnp.zeros_like(picks)
    picks[steps * parts : steps * parts + 1, :] = jnp.sum(spread, axis=0, keepdims=True)
    picked = jnp.dot(chosen.astype(F32).astype(BF16), emb[...], preferred_element_type=F32)
    for t in range(steps):
        for j in range(parts):
            picks[t * parts + j : t * parts + j + 1, :] = picked[t : t + 1, j * LANES : (j + 1) * LANES]
    win_out[...] = picks[...].astype(BF16)

    block = 128
    for at in range(0, rows, block):
        hit = (iota((block, slots), 0) + at) == slot
        mine = jnp.sum(jnp.where(hit, row_quality, 0.0), axis=1, keepdims=True)
        hot = jnp.where(hit, 1.0, 0.0).astype(BF16)
        pair = slice(at // 2, (at + block) // 2)
        moved = jnp.dot(hot, emb[...], preferred_element_type=F32).astype(BF16)
        out[pair, :, :width] = moved.reshape(block // 2, 2, width)
        mine = jnp.broadcast_to(mine, (block, LANES)).astype(BF16)
        out[pair, :, width:] = mine.reshape(block // 2, 2, LANES)


def arrive(rows, relaid, stats, extra):
    balanced, width = relaid.shape
    nt = (((1,), (1,)), ((), ()))
    block = 128
    for at in range(0, balanced, block):
        moved = rows[at // 2 : (at + block) // 2].reshape(block, width + LANES)
        relaid[at : at + block, :] = moved[:, :width]
        extra[at : at + block, :] = moved[:, width:]
    partial = jnp.zeros((balanced, LANES), F32)
    for j in range(width // LANES):
        x = relaid[:, j * LANES : (j + 1) * LANES].astype(F32)
        partial = partial + x * x
    ones = jnp.ones((8, LANES), BF16)
    norms = jnp.zeros((8, balanced), F32)
    rest = partial
    for _ in range(3):
        part = rest.astype(BF16)
        rest = rest - part.astype(F32)
        norms = norms + lax.dot_general(ones, part, nt, preferred_element_type=F32)
    first = jnp.where(iota((8, LANES), 1) == 0, 1.0, 0.0).astype(BF16)
    quality = lax.dot_general(first, extra[...], nt, preferred_element_type=F32)[0:1, :]
    stats[...] = jnp.zeros_like(stats)
    stats[0:1, :] = quality
    stats[1:2, :] = jnp.where(quality > 0, quality * quality * norms[0:1, :] / width + RIDGE, 0.0)


def select(winners, base, rows, stats, side, gain_out, chol_out, wide):
    balanced = stats.shape[1]
    width = wide.shape[1]
    steps = chol_out.shape[0]
    parts = width // LANES
    wide[...] = jnp.zeros_like(wide)
    received = side[...].astype(F32)
    for t in range(steps):
        for j in range(parts):
            wide[t : t + 1, j * LANES : (j + 1) * LANES] = received[t * parts + j : t * parts + j + 1, :]
    win = wide[...].astype(BF16)
    nt = (((1,), (1,)), ((), ()))
    block = 128
    dots = []
    for at in range(0, balanced, block):
        moved = rows[at // 2 : (at + block) // 2, :, :width].reshape(block, width)
        dots.append(lax.dot_general(win, moved, nt, preferred_element_type=F32))
    dots = jnp.concatenate(dots, axis=1)
    gram = lax.dot_general(win, win, nt, preferred_element_type=F32)
    quality = stats[0:1, :]

    scalars = received[steps * parts : steps * parts + 1, :]
    win_quality = [scalars[:, t : 1 + t] for t in range(steps)]
    win_dest = [scalars[:, steps + t : 1 + steps + t].astype(jnp.int32) for t in range(steps)]
    win_rank = [scalars[:, 2 * steps + t : 1 + 2 * steps + t].astype(jnp.int32) for t in range(steps)]

    gain = stats[1:2, :]
    local = iota((1, balanced), 1) + 2 * base[0]
    columns, roots, chol = [], [], []
    for t in range(steps):
        column = []
        for k in range(t):
            cross = win_quality[k] * win_quality[t] * gram[k : k + 1, t : t + 1] / width
            for e in range(k):
                cross = cross - columns[k][e] * column[e]
            column.append(cross / roots[k])
        own_gain = win_quality[t] * win_quality[t] * gram[t : t + 1, t : t + 1] / width + RIDGE
        for k in range(t):
            own_gain = own_gain - column[k] * column[k]
        root = jnp.sqrt(own_gain)
        inner = jnp.zeros((1, balanced), F32)
        for k in range(t):
            inner = inner + chol[k] * column[k]
        place = win_dest[t] * balanced + winners[t] // (balanced // 2) * 2 + win_rank[t]
        hit = jnp.where(local == place, RIDGE, 0.0)
        entry = (quality * win_quality[t] * dots[t : t + 1, :] / width + hit - inner) / root
        gain = gain - entry * entry
        columns.append(column)
        roots.append(root)
        chol.append(entry)
        chol_out[t : t + 1, :] = entry
    gain_out[...] = gain


def gathered(x, axis, rounds):
    size = lax.axis_size(axis)
    for shifts in rounds:
        came = [lax.ppermute(x, axis, [(i, (i + k) % size) for i in range(size)]) for k in shifts]
        for y in came:
            x = x + y
    return x


def along_ring(x):
    ring = lax.axis_size("z")
    total = None
    for k in range(1, ring // 2 + 1):
        back = k % (ring // 2)
        moves = []
        for i in range(ring):
            moves.append((2 * i, 2 * ((i + k) % ring)))
            moves.append((2 * i + 1, 2 * ((i - back) % ring) + 1))
        came = lax.ppermute(x, ("z", "core"), moves)
        total = came if total is None else total + came
    return total


def body(embeds, quality, domain_ids, domain_weight, dest, counts, winners):
    shards = lax.axis_size(ALL)
    slots, width = embeds.shape
    steps = winners.shape[0]
    balanced = 2 * slots
    base = (lax.axis_index(ALL) * slots).reshape(1)
    broad = width + LANES
    held = steps * (width // LANES) + 8

    send, win = pl.pallas_call(
        place,
        in_specs=[SMEM, SMEM, SMEM, SMEM, VMEM, VMEM, VMEM, VMEM],
        out_specs=[VMEM, VMEM],
        out_shape=[
            jax.ShapeDtypeStruct((shards, 2, broad), BF16),
            jax.ShapeDtypeStruct((held, LANES), BF16),
        ],
        scratch_shapes=[pltpu.VMEM((held, LANES), F32)],
        name="place",
    )(
        base,
        winners,
        counts,
        domain_weight,
        embeds,
        dest.reshape(1, slots),
        quality.reshape(1, slots),
        domain_ids.reshape(1, slots),
    )
    rows = lax.all_to_all(send, ALL, 0, 0, tiled=True)
    win = gathered(win, "core", ((1,),))
    win = gathered(win, "y", ((1, 2, 3),))
    win = gathered(win, "x", ((1, 2, 3),))
    win = along_ring(win)
    win = gathered(win, "core", ((1,),))
    small = pltpu.CompilerParams(vmem_limit_bytes=12 << 20)
    relaid, stats = pl.pallas_call(
        arrive,
        in_specs=[VMEM],
        out_specs=[VMEM, VMEM],
        out_shape=[
            jax.ShapeDtypeStruct((balanced, width), BF16),
            jax.ShapeDtypeStruct((8, balanced), F32),
        ],
        scratch_shapes=[pltpu.VMEM((balanced, LANES), BF16)],
        compiler_params=small,
        name="arrive",
    )(rows)
    gain, chol = pl.pallas_call(
        select,
        in_specs=[SMEM, SMEM, VMEM, VMEM, VMEM],
        out_specs=[VMEM, VMEM],
        out_shape=[
            jax.ShapeDtypeStruct((1, balanced), F32),
            jax.ShapeDtypeStruct((steps, balanced), F32),
        ],
        scratch_shapes=[pltpu.VMEM((8, width), F32)],
        compiler_params=small,
        name="select",
    )(winners, base, rows, stats, win)
    return relaid, gain.reshape(balanced), chol


def solution(mesh):
    finer = Mesh(mesh.devices.reshape(8, 4, 4, mesh.shape["grp"]), ALL)
    placed = (P(ALL, None), P(ALL), P(ALL), P(), P(ALL), P(ALL), P())
    return jax.shard_map(
        body,
        mesh=finer,
        in_specs=placed,
        out_specs=(P(ALL, None), P(ALL), P(None, ALL)),
        check_vma=False,
    )
```

```python
import jax
import jax.numpy as jnp
from jax import lax
from jax.experimental import pallas as pl
from jax.experimental.pallas import tpu as pltpu
from jax.sharding import Mesh
from jax.sharding import PartitionSpec as P

ALL = ("z", "x", "y", "core")
RIDGE = 0.1
LANES = 128
F32 = jnp.float32
BF16 = jnp.bfloat16
VMEM = pl.BlockSpec(memory_space=pltpu.VMEM)
SMEM = pl.BlockSpec(memory_space=pltpu.SMEM)


def iota(shape, dim):
    return lax.broadcasted_iota(jnp.int32, shape, dim)


def place(base, winners, counts, weight, emb_in, dest, quality, domain, out, win_out, emb, sem):
    copy = pltpu.make_async_copy(emb_in, emb, sem)
    copy.start()
    slots, width = emb.shape
    rows = 2 * out.shape[0]
    steps = winners.shape[0]
    square = (slots, slots)
    row, col = iota(square, 0), iota(square, 1)
    dest_row = dest[...].astype(F32)
    across = jnp.broadcast_to(dest_row, square)
    down = jnp.sum(jnp.where(row == col, across, 0.0), axis=1, keepdims=True)
    earlier = (down == across) & (row < col)
    rank = jnp.sum(jnp.where(earlier, 1.0, 0.0), axis=0, keepdims=True)
    lane = iota((1, slots), 1)
    valid = lane < counts[0]
    slot = jnp.where(valid, 2 * dest[...] + rank.astype(jnp.int32), -1)
    scale = jnp.zeros((1, slots), F32)
    for k in range(weight.shape[0]):
        scale = jnp.where(domain[...] == k, weight[k], scale)
    row_quality = (quality[...] * scale).astype(BF16).astype(F32)

    turn = iota((8, slots), 0)
    wanted = jnp.full((8, slots), -1, jnp.int32)
    for t in range(steps):
        wanted = jnp.where(turn == t, winners[t] - base[0], wanted)
    chosen = (iota((8, slots), 1) == wanted) & valid
    spread = jnp.zeros((8, LANES), F32)
    turn_out, lane_out = iota((8, LANES), 0), iota((8, LANES), 1)
    for k, value in enumerate((row_quality, dest_row, rank)):
        mine = jnp.sum(jnp.where(chosen, value, 0.0), axis=1, keepdims=True)
        here = (lane_out == k) & (turn_out < steps)
        spread = spread + jnp.where(here, mine, 0.0)
    copy.wait()
    picked = jnp.dot(chosen.astype(F32).astype(BF16), emb[...], preferred_element_type=F32)
    win_out[:, :width] = picked.astype(BF16)
    win_out[:, width:] = spread.astype(BF16)

    block = 128
    for at in range(0, rows, block):
        hit = (iota((block, slots), 0) + at) == slot
        mine = jnp.sum(jnp.where(hit, row_quality, 0.0), axis=1, keepdims=True)
        hot = jnp.where(hit, 1.0, 0.0).astype(BF16)
        pair = slice(at // 2, (at + block) // 2)
        moved = jnp.dot(hot, emb[...], preferred_element_type=F32).astype(BF16)
        out[pair, :, :width] = moved.reshape(block // 2, 2, width)
        mine = jnp.broadcast_to(mine, (block, LANES)).astype(BF16)
        out[pair, :, width:] = mine.reshape(block // 2, 2, LANES)


def select(winners, base, rows, side, relaid, gain_out, chol_out, extra):
    balanced, width = relaid.shape
    steps = chol_out.shape[0]
    parts = width // LANES
    win = side[:, :width]
    nt = (((1,), (1,)), ((), ()))
    block = 128
    for at in range(0, balanced, block):
        moved = rows[at // 2 : (at + block) // 2].reshape(block, width + LANES)
        relaid[at : at + block, :] = moved[:, :width]
        extra[at : at + block, :] = moved[:, width:]
    dots = lax.dot_general(win, relaid[...], nt, preferred_element_type=F32)
    gram = lax.dot_general(win, win, nt, preferred_element_type=F32)
    partial = jnp.zeros((balanced, LANES), F32)
    for j in range(parts):
        x = relaid[:, j * LANES : (j + 1) * LANES].astype(F32)
        partial = partial + x * x
    ones = jnp.ones((8, LANES), BF16)
    norms = jnp.zeros((8, balanced), F32)
    rest = partial
    for _ in range(3):
        part = rest.astype(BF16)
        rest = rest - part.astype(F32)
        norms = norms + lax.dot_general(ones, part, nt, preferred_element_type=F32)
    norms = norms[0:1, :]
    first = jnp.where(iota((8, LANES), 1) == 0, 1.0, 0.0).astype(BF16)
    quality = lax.dot_general(first, extra[...], nt, preferred_element_type=F32)[0:1, :]

    scalars = side[:, width:].astype(F32)
    win_quality = [scalars[t : t + 1, 0:1] for t in range(steps)]
    win_dest = [scalars[t : t + 1, 1:2].astype(jnp.int32) for t in range(steps)]
    win_rank = [scalars[t : t + 1, 2:3].astype(jnp.int32) for t in range(steps)]

    gain = jnp.where(quality > 0, quality * quality * norms / width + RIDGE, 0.0)
    local = iota((1, balanced), 1) + 2 * base[0]
    columns, roots, chol = [], [], []
    for t in range(steps):
        column = []
        for k in range(t):
            cross = win_quality[k] * win_quality[t] * gram[k : k + 1, t : t + 1] / width
            for e in range(k):
                cross = cross - columns[k][e] * column[e]
            column.append(cross / roots[k])
        own_gain = win_quality[t] * win_quality[t] * gram[t : t + 1, t : t + 1] / width + RIDGE
        for k in range(t):
            own_gain = own_gain - column[k] * column[k]
        root = jnp.sqrt(own_gain)
        inner = jnp.zeros((1, balanced), F32)
        for k in range(t):
            inner = inner + chol[k] * column[k]
        place = win_dest[t] * balanced + winners[t] // (balanced // 2) * 2 + win_rank[t]
        hit = jnp.where(local == place, RIDGE, 0.0)
        entry = (quality * win_quality[t] * dots[t : t + 1, :] / width + hit - inner) / root
        gain = gain - entry * entry
        columns.append(column)
        roots.append(root)
        chol.append(entry)
        chol_out[t : t + 1, :] = entry
    gain_out[...] = gain


def gathered(x, axis, rounds):
    size = lax.axis_size(axis)
    for shifts in rounds:
        came = [lax.ppermute(x, axis, [(i, (i + k) % size) for i in range(size)]) for k in shifts]
        for y in came:
            x = x + y
    return x


def along_ring(x):
    ring = lax.axis_size("z")
    total = None
    for k in range(1, ring // 2 + 1):
        back = k % (ring // 2)
        moves = []
        for i in range(ring):
            moves.append((2 * i, 2 * ((i + k) % ring)))
            moves.append((2 * i + 1, 2 * ((i - back) % ring) + 1))
        came = lax.ppermute(x, ("z", "core"), moves)
        total = came if total is None else total + came
    return total


def body(embeds, quality, domain_ids, domain_weight, dest, counts, winners):
    shards = lax.axis_size(ALL)
    slots, width = embeds.shape
    steps = winners.shape[0]
    balanced = 2 * slots
    base = (lax.axis_index(ALL) * slots).reshape(1)
    broad = width + LANES

    send, win = pl.pallas_call(
        place,
        in_specs=[SMEM, SMEM, SMEM, SMEM, pl.BlockSpec(memory_space=pl.ANY), VMEM, VMEM, VMEM],
        out_specs=[VMEM, VMEM],
        out_shape=[
            jax.ShapeDtypeStruct((shards, 2, broad), BF16),
            jax.ShapeDtypeStruct((8, broad), BF16),
        ],
        scratch_shapes=[pltpu.VMEM((slots, width), BF16), pltpu.SemaphoreType.DMA],

        name="place",
    )(
        base,
        winners,
        counts,
        domain_weight,
        embeds,
        dest.reshape(1, slots),
        quality.reshape(1, slots),
        domain_ids.reshape(1, slots),
    )
    rows = lax.all_to_all(send, ALL, 0, 0, tiled=True)
    win = gathered(win, "core", ((1,),))
    win = gathered(win, "y", ((1, 2, 3),))
    win = gathered(win, "x", ((1, 2, 3),))
    win = gathered(along_ring(win), "core", ((1,),))
    relaid, gain, chol = pl.pallas_call(
        select,
        in_specs=[SMEM, SMEM, VMEM, VMEM],
        out_specs=[VMEM, VMEM, VMEM],
        out_shape=[
            jax.ShapeDtypeStruct((balanced, width), BF16),
            jax.ShapeDtypeStruct((1, balanced), F32),
            jax.ShapeDtypeStruct((steps, balanced), F32),
        ],
        scratch_shapes=[pltpu.VMEM((balanced, LANES), BF16)],
        compiler_params=pltpu.CompilerParams(vmem_limit_bytes=12 << 20),
        name="select",
    )(winners, base, rows, win)
    return relaid, gain.reshape(balanced), chol


def solution(mesh):
    finer = Mesh(mesh.devices.reshape(8, 4, 4, mesh.shape["grp"]), ALL)
    placed = (P(ALL, None), P(ALL), P(ALL), P(), P(ALL), P(ALL), P())
    return jax.shard_map(
        body,
        mesh=finer,
        in_specs=placed,
        out_specs=(P(ALL, None), P(ALL), P(None, ALL)),
        check_vma=False,
    )
```

```python
import jax
import jax.numpy as jnp
from jax import lax
from jax.experimental import pallas as pl
from jax.experimental.pallas import tpu as pltpu
from jax.sharding import Mesh
from jax.sharding import PartitionSpec as P

ALL = ("z", "x", "y", "core")
RIDGE = 0.1
LANES = 128
F32 = jnp.float32
BF16 = jnp.bfloat16
VMEM = pl.BlockSpec(memory_space=pltpu.VMEM)
SMEM = pl.BlockSpec(memory_space=pltpu.SMEM)


def iota(shape, dim):
    return lax.broadcasted_iota(jnp.int32, shape, dim)


def place(base, winners, counts, weight, emb, dest, quality, domain, out, win_out):
    slots, width = emb.shape
    rows = 2 * out.shape[0]
    steps = winners.shape[0]
    square = (slots, slots)
    row, col = iota(square, 0), iota(square, 1)
    dest_row = dest[...].astype(F32)
    across = jnp.broadcast_to(dest_row, square)
    down = jnp.sum(jnp.where(row == col, across, 0.0), axis=1, keepdims=True)
    earlier = (down == across) & (row < col)
    rank = jnp.sum(jnp.where(earlier, 1.0, 0.0), axis=0, keepdims=True)
    lane = iota((1, slots), 1)
    valid = lane < counts[0]
    slot = jnp.where(valid, 2 * dest[...] + rank.astype(jnp.int32), -1)
    scale = jnp.zeros((1, slots), F32)
    for k in range(weight.shape[0]):
        scale = jnp.where(domain[...] == k, weight[k], scale)
    row_quality = (quality[...] * scale).astype(BF16).astype(F32)

    turn = iota((8, slots), 0)
    wanted = jnp.full((8, slots), -1, jnp.int32)
    for t in range(steps):
        wanted = jnp.where(turn == t, winners[t] - base[0], wanted)
    chosen = (iota((8, slots), 1) == wanted) & valid
    spread = jnp.zeros((8, LANES), F32)
    turn_out, lane_out = iota((8, LANES), 0), iota((8, LANES), 1)
    for k, value in enumerate((row_quality, dest_row, rank)):
        mine = jnp.sum(jnp.where(chosen, value, 0.0), axis=1, keepdims=True)
        here = (lane_out == k) & (turn_out < steps)
        spread = spread + jnp.where(here, mine, 0.0)
    picked = jnp.dot(chosen.astype(F32).astype(BF16), emb[...], preferred_element_type=F32)
    win_out[:, :width] = picked.astype(BF16)
    win_out[:, width:] = spread.astype(BF16)

    block = 128
    for at in range(0, rows, block):
        hit = (iota((block, slots), 0) + at) == slot
        mine = jnp.sum(jnp.where(hit, row_quality, 0.0), axis=1, keepdims=True)
        hot = jnp.where(hit, 1.0, 0.0).astype(BF16)
        pair = slice(at // 2, (at + block) // 2)
        moved = jnp.dot(hot, emb[...], preferred_element_type=F32).astype(BF16)
        out[pair, :, :width] = moved.reshape(block // 2, 2, width)
        mine = jnp.broadcast_to(mine, (block, LANES)).astype(BF16)
        out[pair, :, width:] = mine.reshape(block // 2, 2, LANES)


def select(winners, base, rows, side, relaid, gain_out, chol_out, extra):
    balanced, width = relaid.shape
    steps = chol_out.shape[0]
    parts = width // LANES
    win = side[:, :width]
    nt = (((1,), (1,)), ((), ()))
    block = 128
    for at in range(0, balanced, block):
        moved = rows[at // 2 : (at + block) // 2].reshape(block, width + LANES)
        relaid[at : at + block, :] = moved[:, :width]
        extra[at : at + block, :] = moved[:, width:]
    dots = lax.dot_general(win, relaid[...], nt, preferred_element_type=F32)
    gram = lax.dot_general(win, win, nt, preferred_element_type=F32)
    partial = jnp.zeros((balanced, LANES), F32)
    for j in range(parts):
        x = relaid[:, j * LANES : (j + 1) * LANES].astype(F32)
        partial = partial + x * x
    ones = jnp.ones((8, LANES), BF16)
    norms = jnp.zeros((8, balanced), F32)
    rest = partial
    for _ in range(3):
        part = rest.astype(BF16)
        rest = rest - part.astype(F32)
        norms = norms + lax.dot_general(ones, part, nt, preferred_element_type=F32)
    norms = norms[0:1, :]
    first = jnp.where(iota((8, LANES), 1) == 0, 1.0, 0.0).astype(BF16)
    quality = lax.dot_general(first, extra[...], nt, preferred_element_type=F32)[0:1, :]

    scalars = side[:, width:].astype(F32)
    win_quality = [scalars[t : t + 1, 0:1] for t in range(steps)]
    win_dest = [scalars[t : t + 1, 1:2].astype(jnp.int32) for t in range(steps)]
    win_rank = [scalars[t : t + 1, 2:3].astype(jnp.int32) for t in range(steps)]

    gain = jnp.where(quality > 0, quality * quality * norms / width + RIDGE, 0.0)
    local = iota((1, balanced), 1) + 2 * base[0]
    columns, roots, chol = [], [], []
    for t in range(steps):
        column = []
        for k in range(t):
            cross = win_quality[k] * win_quality[t] * gram[k : k + 1, t : t + 1] / width
            for e in range(k):
                cross = cross - columns[k][e] * column[e]
            column.append(cross / roots[k])
        own_gain = win_quality[t] * win_quality[t] * gram[t : t + 1, t : t + 1] / width + RIDGE
        for k in range(t):
            own_gain = own_gain - column[k] * column[k]
        root = jnp.sqrt(own_gain)
        inner = jnp.zeros((1, balanced), F32)
        for k in range(t):
            inner = inner + chol[k] * column[k]
        place = win_dest[t] * balanced + winners[t] // (balanced // 2) * 2 + win_rank[t]
        hit = jnp.where(local == place, RIDGE, 0.0)
        entry = (quality * win_quality[t] * dots[t : t + 1, :] / width + hit - inner) / root
        gain = gain - entry * entry
        columns.append(column)
        roots.append(root)
        chol.append(entry)
        chol_out[t : t + 1, :] = entry
    gain_out[...] = gain


def gathered(x, axis, rounds):
    size = lax.axis_size(axis)
    for shifts in rounds:
        came = [lax.ppermute(x, axis, [(i, (i + k) % size) for i in range(size)]) for k in shifts]
        for y in came:
            x = x + y
    return x


def along_ring(x):
    ring = lax.axis_size("z")
    total = None
    for k in range(1, ring // 2 + 1):
        back = k % (ring // 2)
        moves = []
        for i in range(ring):
            moves.append((2 * i, 2 * ((i + k) % ring)))
            moves.append((2 * i + 1, 2 * ((i - back) % ring) + 1))
        came = lax.ppermute(x, ("z", "core"), moves)
        total = came if total is None else total + came
    return total


def body(embeds, quality, domain_ids, domain_weight, dest, counts, winners):
    shards = lax.axis_size(ALL)
    slots, width = embeds.shape
    steps = winners.shape[0]
    balanced = 2 * slots
    base = (lax.axis_index(ALL) * slots).reshape(1)
    broad = width + LANES

    send, win = pl.pallas_call(
        place,
        in_specs=[SMEM, SMEM, SMEM, SMEM, VMEM, VMEM, VMEM, VMEM],
        out_specs=[VMEM, VMEM],
        out_shape=[
            jax.ShapeDtypeStruct((shards, 2, broad), BF16),
            jax.ShapeDtypeStruct((8, broad), BF16),
        ],

        name="place",
    )(
        base,
        winners,
        counts,
        domain_weight,
        embeds,
        dest.reshape(1, slots),
        quality.reshape(1, slots),
        domain_ids.reshape(1, slots),
    )
    rows = lax.all_to_all(send, ALL, 0, 0, tiled=True)
    win = gathered(win, "core", ((1,),))
    win = gathered(win, "y", ((1, 2, 3),))
    win = gathered(win, "x", ((1, 2, 3),))
    win = gathered(along_ring(win), "core", ((1,),))
    relaid, gain, chol = pl.pallas_call(
        select,
        in_specs=[SMEM, SMEM, VMEM, VMEM],
        out_specs=[VMEM, VMEM, VMEM],
        out_shape=[
            jax.ShapeDtypeStruct((balanced, width), BF16),
            jax.ShapeDtypeStruct((1, balanced), F32),
            jax.ShapeDtypeStruct((steps, balanced), F32),
        ],
        scratch_shapes=[pltpu.VMEM((balanced, LANES), BF16)],
        compiler_params=pltpu.CompilerParams(vmem_limit_bytes=12 << 20),
        name="select",
    )(winners, base, rows, win)
    return relaid, gain.reshape(balanced), chol


def solution(mesh):
    finer = Mesh(mesh.devices.reshape(8, 4, 4, mesh.shape["grp"]), ALL)
    placed = (P(ALL, None), P(ALL), P(ALL), P(), P(ALL), P(ALL), P())
    return jax.shard_map(
        body,
        mesh=finer,
        in_specs=placed,
        out_specs=(P(ALL, None), P(ALL), P(None, ALL)),
        check_vma=False,
    )
```
